128 devices in a mesh: leaf: 32 (over y, x, core), rhs: 4 (over z).
Axes of the slice: x: 4, y: 4, z: 4, core: 2. Of those that a mesh axis runs over, the one named last changes fastest.
Arguments:
- rhs_cols: bfloat16 [262144, 512], P('leaf', 'rhs'), may hold values from -6 to 6
- leaf_inv: bfloat16 [512, 512, 512], P('leaf', 'rhs')
- leaf_basis: bfloat16 [512, 512, 128], P('leaf'), may hold values from -0.25 to 0.25
- leaf_back: bfloat16 [512, 512, 128], P('leaf'), may hold values from -0.5 to 0.5
- leaf_coarse: float32 [512, 128, 128], P('leaf')
- mid_inv: float32 [480, 256, 256], P('leaf')
- mid_basis: float32 [480, 256, 128], P('leaf'), may hold values from -0.375 to 0.375
- mid_back: float32 [480, 256, 128], P('leaf'), may hold values from -0.5 to 0.5
- mid_coarse: float32 [480, 128, 128], P('leaf')
- top_inv: float32 [32, 256, 256], P('leaf')
- top_basis: float32 [32, 256, 128], P('leaf'), may hold values from -0.375 to 0.375
- top_back: float32 [32, 256, 128], P('leaf'), may hold values from -0.5 to 0.5
- top_coarse: float32 [32, 128, 128], P('leaf')
Outputs:
- solution: float32 [262144, 512], P('leaf', 'rhs')
The draws below stay inside these ranges and needn't reach their ends.
All inputs are finite; a program needn't handle non-finite values.
Results may differ from the reference program's by a relative error of at most 0.004.
Values may be sent and summed in bfloat16 or wider, within the bound.
No kernel may reach another device: no remote copies, remote signals or barrier semaphores. Data moves between devices by JAX's collectives and lax.ppermute only.
A program may use at most 192 MiB of HBM per device.

```python
import jax
import jax.numpy as jnp
import numpy as np
from jax import lax

LEAF = 512
RANK = 128
RHS = 512
LEAF_DEV = 16
LEAVES = 512
POINTS = 262144
MIDS = 480
N_LEAF = 32


def dominant(key, count, order, salt):
    first_key, second_key = jax.random.split(jax.random.fold_in(key, salt))
    spread = jax.random.normal(first_key, (count, order, order), jnp.float32) * (0.3 / order ** 0.5)
    diagonal = jax.random.uniform(second_key, (count, order), jnp.float32, 0.7, 1.2)
    identity = jnp.eye(order, dtype=jnp.float32)
    return spread * (1.0 - identity) + identity * diagonal[:, None, :]


def draw_leaf_inv(key, part):
    return dominant(key, LEAVES, LEAF, 101).astype(jnp.bfloat16)


def draw_leaf_coarse(key, part):
    return dominant(key, LEAVES, RANK, 202)


def draw_mid_inv(key, part):
    return dominant(key, MIDS, 2 * RANK, 303)


def draw_mid_coarse(key, part):
    return dominant(key, MIDS, RANK, 404)


def draw_top_inv(key, part):
    return dominant(key, N_LEAF, 2 * RANK, 505)


def draw_top_coarse(key, part):
    return dominant(key, N_LEAF, RANK, 606)


def block_scale(own_key, dims, cuts, smallest, high):
    def one(dim, parts):
        steps = jax.random.uniform(jax.random.fold_in(jax.random.fold_in(own_key, 6), dim), (parts,), jnp.float32, smallest / len(cuts), high / len(cuts))
        return jnp.repeat(jnp.exp(steps), dims[dim] // parts).reshape((-1,) + (1,) * (len(dims) - dim - 1))

    level = one(*cuts[0])
    for cut in cuts[1:]:
        level = level * one(*cut)
    return level


def scatter_about(key, extent, deviation, most, pieces=(), kind=jnp.bfloat16):
    loudness = block_scale(key, extent, pieces, -0.22, 0.18) if pieces else 1.0
    values = jax.random.normal(key, extent, jnp.float32) * deviation * loudness
    return jnp.minimum(jnp.maximum(values, -most), most).astype(kind)


def setup_inputs(seed: int = 0) -> dict:
    key_of = jax.random.split(jax.random.key(seed), 14)
    rhs_cols = scatter_about(key_of[0], (POINTS, RHS), 1.0, 6.0, ((0, 32), (1, 4)))
    leaf_inv = draw_leaf_inv(jax.random.fold_in(key_of[13], 71), 0)
    leaf_basis = scatter_about(key_of[2], (LEAVES, LEAF, RANK), LEAF ** -0.5, 0.25, ((0, 32),))
    leaf_back = scatter_about(key_of[3], (LEAVES, LEAF, RANK), RANK ** -0.5, 0.5, ((0, 32),))
    leaf_coarse = draw_leaf_coarse(jax.random.fold_in(key_of[13], 71), 0)
    mid_inv = draw_mid_inv(jax.random.fold_in(key_of[13], 71), 0)
    mid_basis = scatter_about(key_of[6], (MIDS, 2 * RANK, RANK), (2 * RANK) ** -0.5, 0.375, ((0, 32),), jnp.float32)
    mid_back = scatter_about(key_of[7], (MIDS, 2 * RANK, RANK), RANK ** -0.5, 0.5, ((0, 32),), jnp.float32)
    mid_coarse = draw_mid_coarse(jax.random.fold_in(key_of[13], 71), 0)
    top_inv = draw_top_inv(jax.random.fold_in(key_of[13], 71), 0)
    top_basis = scatter_about(key_of[10], (N_LEAF, 2 * RANK, RANK), (2 * RANK) ** -0.5, 0.375, ((0, 32),), jnp.float32)
    top_back = scatter_about(key_of[11], (N_LEAF, 2 * RANK, RANK), RANK ** -0.5, 0.5, ((0, 32),), jnp.float32)
    top_coarse = draw_top_coarse(jax.random.fold_in(key_of[13], 71), 0)
    return dict(rhs_cols=rhs_cols, leaf_inv=leaf_inv, leaf_basis=leaf_basis, leaf_back=leaf_back, leaf_coarse=leaf_coarse, mid_inv=mid_inv, mid_basis=mid_basis, mid_back=mid_back, mid_coarse=mid_coarse, top_inv=top_inv, top_basis=top_basis, top_back=top_back, top_coarse=top_coarse)


exact_mode = lax.Precision.HIGHEST


def node_up(inverse, basis_mat, coarse, stacked):
    solved = jnp.einsum('nij,njc->nic', inverse, stacked, precision=exact_mode)
    reduced = jnp.einsum('nik,nic->nkc', basis_mat, solved, precision=exact_mode)
    upward = jnp.einsum('nkl,nlc->nkc', coarse, reduced, precision=exact_mode)
    return solved, reduced, upward


def node_down(solved, reduced, back_mat, parent_part):
    return solved - jnp.einsum('nik,nkc->nic', back_mat, reduced - parent_part, precision=exact_mode)


def leaf_solve(operands):
    inverse, block = operands
    return jnp.dot(inverse, block, preferred_element_type=jnp.float32).astype(jnp.bfloat16)


def reference(rhs_cols, leaf_inv, leaf_basis, leaf_back, leaf_coarse, mid_inv, mid_basis, mid_back, mid_coarse, top_inv, top_basis, top_back, top_coarse):
    blocks = rhs_cols.reshape(LEAVES, LEAF, RHS)
    leaf_vals = lax.map(leaf_solve, (leaf_inv, blocks))
    leaf_proj = jnp.einsum('nik,nic->nkc', leaf_basis.astype(jnp.float32), leaf_vals.astype(jnp.float32))
    current = jnp.einsum('nkl,nlc->nkc', leaf_coarse, leaf_proj, precision=exact_mode)
    local_levels = LEAF_DEV.bit_length() - 1
    top_levels = N_LEAF.bit_length() - 1
    total_levels = local_levels + top_levels
    stored = []
    for height in range(1, total_levels + 1):
        node_count = LEAVES >> height
        if height <= local_levels:
            per_device = LEAF_DEV >> height
            offset = LEAF_DEV - (LEAF_DEV >> (height - 1))
            index = np.array([(p // per_device) * (LEAF_DEV - 1) + offset + p % per_device for p in range(node_count)], dtype=np.int32)
            factors = (mid_inv[index], mid_basis[index], mid_back[index], mid_coarse[index])
        else:
            upper = height - local_levels
            index = np.arange(node_count, dtype=np.int32) * (1 << upper) + (1 << (upper - 1))
            factors = (top_inv[index], top_basis[index], top_back[index], top_coarse[index])
        stacked = current.reshape(node_count, 2 * RANK, RHS)
        solved, reduced, current = node_up(factors[0], factors[1], factors[2 + 1], stacked)
        stored.append((solved, reduced, factors[2]))
    parent_part = None
    for height in range(total_levels, 0, -1):
        solved, reduced, back_mat = stored[height - 1]
        if height == total_levels:
            halves = solved
        else:
            halves = node_down(solved, reduced, back_mat, parent_part)
        parent_part = halves.reshape(2 * halves.shape[0], RANK, RHS)
    difference = (leaf_proj - parent_part).astype(jnp.bfloat16)
    result = leaf_vals.astype(jnp.float32) - jnp.einsum('nik,nkc->nic', leaf_back.astype(jnp.float32), difference.astype(jnp.float32))
    return result.reshape(POINTS, RHS)
```

```python
import jax
import jax.numpy as jnp
from jax import lax
from jax.experimental import pallas as pl
from jax.experimental.pallas import tpu as pltpu
from jax.sharding import PartitionSpec as P


exact_mode = lax.Precision.HIGHEST
wide = jnp.float32
narrow = jnp.bfloat16

GROUPS = ((0, 8), (8, 4), (12, 4))
NODE_ROWS = ((0, 1, 2, 3, 8, 9, 12), (4, 5, 10), (6, 7, 11, 13, 14))
MERGES = (
    (("g", 0, 1), ("g", 2, 3), ("g", 4, 5), ("g", 6, 7), ("u", 0, 1), ("u", 2, 3), ("u", 4, 5)),
    (("g", 0, 1), ("g", 2, 3), ("u", 0, 1)),
    (("g", 0, 1), ("g", 2, 3), ("u", 0, 1), ("x1", 2, 2), ("x0", 6, 3)),
)


def narrow_dot(a, b):
    return jnp.dot(a.astype(narrow), b.astype(narrow), preferred_element_type=wide)


def parts_of(a):
    high = a.astype(narrow)
    return high, (a - high.astype(wide)).astype(narrow)


def split_dot(a, b):
    a_high, a_low = parts_of(a)
    b_high, b_low = parts_of(b)
    return (
        jnp.dot(a_high, b_low, preferred_element_type=wide)
        + jnp.dot(a_low, b_high, preferred_element_type=wide)
        + jnp.dot(a_high, b_high, preferred_element_type=wide)
    )


def close_dot(a, b):
    return jnp.dot(a, b, precision=lax.Precision.HIGH, preferred_element_type=wide)


def full_spec(array):
    rank = array.ndim
    return pl.BlockSpec(array.shape, lambda i, row: (0,) * rank)


def leaf_body(which, *refs):
    start, count = GROUPS[which]
    merges = MERGES[which]
    (row_ref, own, left, right, far_a, far_b, rhs, basis, coarse, ups, *more) = refs
    if which == 0:
        (downs, vals, proj, lead, up, solved) = more
    elif which == 1:
        (downs, _, _, vals, proj, lead, up, solved) = more
    else:
        (earlier0, earlier1, _, _, vals, proj, lead, up) = more
    step = pl.program_id(0)
    row = row_ref[0]
    block = rhs[...]
    height = own.shape[1]

    def put(rows, part):
        at = pl.multiple_of(lax.rem(row + part, 4) * height, height)
        vals[0, pl.ds(at, height), :] = narrow_dot(rows, block).astype(narrow)

    put(own[0], 0)
    put(left[0], 3)
    put(right[0], 1)
    put(jnp.where(step < count // 2, far_a[0], far_b[0]), 2)
    reduced = lax.dot_general(
        basis[0], vals[0], (((0,), (0,)), ((), ())), preferred_element_type=wide
    )
    proj[0] = reduced
    lead[step] = split_dot(coarse[0], reduced)

    @pl.when(step == count - 1)
    def _():
        for k, (kind, a, b) in enumerate(merges):
            if kind == "g":
                pair = (lead[a], lead[b])
            elif kind == "u":
                pair = (up[a], up[b])
            elif kind == "x1":
                pair = (earlier1[a], up[b])
            else:
                pair = (earlier0[a], up[b])
            stacked = jnp.concatenate(pair, axis=0)
            up[k] = split_dot(ups[k], stacked)
            if which < 2:
                solved[k] = split_dot(downs[k], stacked)


def leaf_call(which, row, own, left, right, far_a, far_b, rhs, basis, coarse, ups, extra, kept):
    start, count = GROUPS[which]
    half = count // 2
    base = 0 if which == 0 else 8
    nodes = len(MERGES[which])
    height, width = own.shape[1], own.shape[2]
    rank, columns = basis.shape[2], rhs.shape[1]
    leaves = own.shape[0]
    in_specs = [
        pl.BlockSpec((1, height, width), lambda i, row: (start + i, 0, 0)),
        pl.BlockSpec((1, height, width), lambda i, row: (start - base + i, 0, 0)),
        pl.BlockSpec((1, height, width), lambda i, row: (start - base + i, 0, 0)),
        pl.BlockSpec((1, height, width), lambda i, row: (jnp.minimum(i, half - 1), 0, 0)),
        pl.BlockSpec((1, height, width), lambda i, row: (jnp.maximum(i - half, 0), 0, 0)),
        pl.BlockSpec((width, columns), lambda i, row: (start + i, 0)),
        pl.BlockSpec((1, width, rank), lambda i, row: (start + i, 0, 0)),
        pl.BlockSpec((1, rank, rank), lambda i, row: (start + i, 0, 0)),
        full_spec(ups),
    ] + [full_spec(e) for e in extra] + [pl.BlockSpec(memory_space=pl.ANY) for _ in kept]
    out_shape = [
        jax.ShapeDtypeStruct((leaves, width, columns), narrow),
        jax.ShapeDtypeStruct((leaves, rank, columns), wide),
        jax.ShapeDtypeStruct((count, rank, columns), wide),
        jax.ShapeDtypeStruct((nodes, rank, columns), wide),
    ]
    out_specs = [
        pl.BlockSpec((1, width, columns), lambda i, row: (start + i, 0, 0)),
        pl.BlockSpec((1, rank, columns), lambda i, row: (start + i, 0, 0)),
        full_spec(out_shape[2]),
        full_spec(out_shape[3]),
    ]
    if which < 2:
        out_shape.append(jax.ShapeDtypeStruct((nodes, 2 * rank, columns), wide))
        out_specs.append(full_spec(out_shape[4]))
    first = 10 + len(extra)
    aliases = {first + k: k for k in range(len(kept))}
    operands = (own, left, right, far_a, far_b, rhs, basis, coarse, ups, *extra, *kept)

    def body(*refs):
        leaf_body(which, *refs)

    return pl.pallas_call(
        body,
        grid_spec=pltpu.PrefetchScalarGridSpec(
            num_scalar_prefetch=1, grid=(count,), in_specs=in_specs, out_specs=out_specs
        ),
        out_shape=out_shape,
        input_output_aliases=aliases,
        cost_estimate=pl.CostEstimate(
            flops=count * 2 * width * width * columns * 2,
            bytes_accessed=count * (width * width + 3 * width * columns) * 2,
            transcendentals=0,
        ),
        name=f"leaf_group_{which}",
    )(row, *operands)


def down_body(lead, up, earlier0, earlier1, solved0, solved1, downs, backs, proj, rest):
    rank = proj.shape[1]
    solved = {}
    for slot, node in enumerate(NODE_ROWS[0]):
        solved[node] = solved0[slot]
    for slot, node in enumerate(NODE_ROWS[1]):
        solved[node] = solved1[slot]
    pairs = (
        (lead[0], lead[1]),
        (lead[2], lead[3]),
        (up[0], up[1]),
        (earlier1[2], up[2]),
        (earlier0[6], up[3]),
    )
    for slot, node in enumerate(NODE_ROWS[2]):
        solved[node] = split_dot(downs[slot], jnp.concatenate(pairs[slot], axis=0))
    parts = [None]
    for offset, count in ((14, 1), (12, 2), (8, 4), (0, 8)):
        below = []
        for k in range(count):
            halves = solved[offset + k]
            if parts[k] is not None:
                halves = halves + split_dot(backs[offset + k], parts[k])
            below += [halves[:rank], halves[rank:]]
        parts = below
    for k, part in enumerate(parts):
        rest[k] = proj[k] - part


def out_body(top_ref, paths, rest, back, vals, out):
    width = back.shape[1]
    top = top_ref[...]
    for k in range(back.shape[0]):
        difference = (rest[k] - split_dot(paths[k], top)).astype(narrow)
        out[pl.ds(k * width, width), :] = vals[k].astype(wide) - narrow_dot(back[k], difference)


def out_call(top, paths, rest, back, vals):
    leaves, width, rank = back.shape
    columns = vals.shape[2]
    some = 2
    return pl.pallas_call(
        out_body,
        grid=(leaves // some,),
        in_specs=[
            pl.BlockSpec(top.shape, lambda i: (0, 0)),
            pl.BlockSpec((some, rank, rank), lambda i: (i, 0, 0)),
            pl.BlockSpec((some, rank, columns), lambda i: (i, 0, 0)),
            pl.BlockSpec((some, width, rank), lambda i: (i, 0, 0)),
            pl.BlockSpec((some, width, columns), lambda i: (i, 0, 0)),
        ],
        out_specs=pl.BlockSpec((some * width, columns), lambda i: (i, 0)),
        out_shape=jax.ShapeDtypeStruct((leaves * width, columns), wide),
        name="leaf_result",
    )(top, paths, rest, back, vals)


def down_call(*operands):
    proj = operands[-1]
    return pl.pallas_call(
        down_body,
        out_shape=jax.ShapeDtypeStruct(proj.shape, wide),
        cost_estimate=pl.CostEstimate(flops=4 * 10**8, bytes_accessed=4 * 10**6, transcendentals=0),
        name="known_part",
    )(*operands)


def node_forms(inverse, basis_mat, back_mat, coarse):
    reduce_mat = jnp.einsum("nik,nij->nkj", basis_mat, inverse, precision=exact_mode)
    up_mat = jnp.einsum("nkl,nlj->nkj", coarse, reduce_mat, precision=exact_mode)
    down_mat = inverse - jnp.einsum("nik,nkj->nij", back_mat, reduce_mat, precision=exact_mode)
    return up_mat, down_mat


def top_factors(package, position, tree_depth):
    total = lax.axis_size("leaf")
    upper = None
    for bit in reversed(range(tree_depth)):
        stride = 1 << bit
        high = (position >> bit) % 2 == 1
        if upper is None:
            pairs = [(stride, 0)]
            message = package
        else:
            pairs = [(i, i ^ stride) for i in range(0, total, stride)]
            pad = jnp.concatenate([package] * upper.shape[0], axis=0)
            message = jnp.where(high, pad, upper)
        received = lax.ppermute(message, "leaf", pairs)
        mine = jnp.where(high, package, received[:1])
        if upper is None:
            upper = mine
        else:
            upper = jnp.concatenate([jnp.where(high, received, upper), mine], axis=0)
    return [upper[tree_depth - height] for height in range(1, tree_depth + 1)]


def per_device(
    rhs_cols,
    leaf_inv,
    leaf_basis,
    leaf_back,
    leaf_coarse,
    mid_inv,
    mid_basis,
    mid_back,
    mid_coarse,
    top_inv,
    top_basis,
    top_back,
    top_coarse,
):
    leaf_count, height, width = leaf_inv.shape
    rank = leaf_basis.shape[2]
    position = lax.axis_index("leaf")
    leaf_total = lax.axis_size("leaf")
    tree_depth = leaf_total.bit_length() - 1
    ring = lax.axis_size("rhs")
    ahead = [(i, (i + 1) % ring) for i in range(ring)]
    behind = [(i, (i - 1) % ring) for i in range(ring)]

    def forth(a):
        return lax.ppermute(a, "rhs", ahead)

    def back(a):
        return lax.ppermute(a, "rhs", behind)

    half = leaf_count // 2
    left, right, far = [], [], []
    for part in range(2):
        own = leaf_inv[part * half : (part + 1) * half]
        left.append(forth(own))
        right.append(back(own))
    q = half // 2
    far.append((forth(left[0][:q]), back(right[0][q:])))
    e = q // 2
    far.append((forth(left[1][:e]), back(right[1][e : 2 * e])))
    far.append((forth(left[1][2 * e : 3 * e]), back(right[1][3 * e :])))

    up_top, down_top = node_forms(top_inv, top_basis, top_back, top_coarse)
    is_root = position == leaf_total // 2
    down_top = jnp.where(is_root, top_inv, down_top)
    package = jnp.concatenate(
        [up_top, down_top, jnp.swapaxes(top_back, 1, 2)], axis=1
    )
    nodes = top_factors(package, position, tree_depth)
    ups_own, ups_sib, path = [], [], None
    for level, node in enumerate(nodes):
        is_left = (position >> level) % 2 == 0
        up_mat = node[:rank]
        down_mat = node[rank : 3 * rank]
        back_mat = node[3 * rank :].T
        down_mat = jnp.where(is_left, down_mat[:rank], down_mat[rank:])
        back_mat = jnp.where(is_left, back_mat[:rank], back_mat[rank:])
        if path is not None:
            down_mat = jnp.dot(path, down_mat, precision=exact_mode)
        both = jnp.concatenate([up_mat, down_mat], axis=0)
        ups_own.append(jnp.where(is_left, both[:, :rank], both[:, rank:]))
        ups_sib.append(jnp.where(is_left, both[:, rank:], both[:, :rank]))
        path = back_mat if path is None else jnp.dot(path, back_mat, precision=exact_mode)

    up_mat, down_mat = node_forms(mid_inv, mid_basis, mid_back, mid_coarse)
    paths = None
    for offset, count in ((14, 1), (12, 2), (8, 4), (0, 8)):
        here = mid_back[offset : offset + count]
        if paths is not None:
            here = jnp.einsum("nik,nkl->nil", here, paths, precision=exact_mode)
        paths = here.reshape(2 * count, rank, rank)

    row = lax.axis_index("rhs").astype(jnp.int32).reshape(1)
    ups = [jnp.stack([up_mat[k] for k in rows]) for rows in NODE_ROWS]
    downs = [jnp.stack([down_mat[k] for k in rows]) for rows in NODE_ROWS]
    shared = (rhs_cols, leaf_basis, leaf_coarse)
    vals, proj, lead0, up0, solved0 = leaf_call(
        0, row, leaf_inv, left[0], right[0], *far[0], *shared, ups[0], (downs[0],), ()
    )
    vals, proj, lead1, up1, solved1 = leaf_call(
        1, row, leaf_inv, left[1], right[1], *far[1], *shared, ups[1], (downs[1],), (vals, proj)
    )
    last = lax.optimization_barrier((far[2], ups_own, ups_sib, paths))
    far[2], ups_own, ups_sib, paths = last
    vals, proj, lead2, up2 = leaf_call(
        2, row, leaf_inv, left[1], right[1], *far[2], *shared, ups[2], (up0, up1), (vals, proj)
    )
    rest = down_call(lead2, up2, up0, up1, solved0, solved1, downs[2], mid_back, proj)

    current = up2[4]
    top = None
    for level in range(tree_depth):
        stride = 1 << level
        partner = lax.ppermute(
            current, "leaf", [(i, i ^ stride) for i in range(leaf_total)]
        )
        both = close_dot(ups_own[level], current) + close_dot(ups_sib[level], partner)
        current = both[:rank]
        top = both[rank:] if top is None else top + both[rank:]
    return out_call(top, paths, rest, leaf_back, vals)


def solution(mesh):
    return jax.shard_map(
        per_device,
        mesh=mesh,
        in_specs=(
            P("leaf", "rhs"),
            P("leaf", "rhs", None),
        )
        + (P("leaf", None, None),) * 11,
        out_specs=P("leaf", "rhs"),
        check_vma=False,
    )
```

```python
import jax
import jax.numpy as jnp
from jax import lax
from jax.experimental import pallas as pl
from jax.experimental.pallas import tpu as pltpu
from jax.sharding import PartitionSpec as P


wide = jnp.float32
narrow = jnp.bfloat16

GROUPS = ((0, 4), (4, 8), (12, 4))
EARLY = (0, 1, 8, 2, 3, 4, 5, 9, 10, 12)
LATE = (6, 7, 11, 13, 14)
FRONT = (((0,), (0,)), ((), ()))


def narrow_dot(a, b):
    return jnp.dot(a.astype(narrow), b.astype(narrow), preferred_element_type=wide)


def parts_of(a):
    high = a.astype(narrow)
    return high, (a - high.astype(wide)).astype(narrow)


def split_dot(a, b, dims=(((1,), (0,)), ((), ()))):
    a_high, a_low = parts_of(a)
    b_high, b_low = parts_of(b)

    def one(p, q):
        return lax.dot_general(p, q, dims, preferred_element_type=wide)

    return one(a_high, b_low) + one(a_low, b_high) + one(a_high, b_high)


def close_dot(a, b):
    return jnp.dot(a, b, precision=lax.Precision.HIGH, preferred_element_type=wide)


def kernel_call(body, out_shape, flops, operands, scalars=0, room=16, **more):
    if scalars:
        more["in_specs"] = [pl.BlockSpec(memory_space=pltpu.SMEM)] * scalars + [
            pl.BlockSpec(a.shape, lambda a=a: (0,) * a.ndim) for a in operands[scalars:]
        ]
    size = sum(a.size * a.dtype.itemsize for a in operands)
    return pl.pallas_call(
        body,
        out_shape=out_shape,
        cost_estimate=pl.CostEstimate(flops=flops, bytes_accessed=size, transcendentals=0),
        compiler_params=pltpu.CompilerParams(vmem_limit_bytes=room * 1024 * 1024),
        **more,
    )(*operands)


def turned(row_ref, part, height):
    return pl.multiple_of(lax.rem(row_ref[0] + part, 4) * height, height)


def near_body(row_ref, own, left, right, rhs, basis, vals, proj):
    count, height, width = own.shape
    for k in range(count):
        rows = jnp.concatenate([own[k], left[k], right[k]], axis=0)
        got = narrow_dot(rows, rhs[k * width : (k + 1) * width, :]).astype(narrow)
        vals[k] = got
        matching = jnp.concatenate(
            [basis[k, pl.ds(turned(row_ref, part, height), height), :] for part in (0, 3, 1)],
            axis=0,
        )
        proj[k] = lax.dot_general(matching, got, FRONT, preferred_element_type=wide)


def near_call(start, row, own, left, right, rhs, basis):
    count, height, width = left.shape
    rank, columns = basis.shape[2], rhs.shape[1]
    some = 2
    base = start // some

    def at(shape, shift):
        return pl.BlockSpec(shape, lambda i, row: (shift + i,) + (0,) * (len(shape) - 1))

    return pl.pallas_call(
        near_body,
        grid_spec=pltpu.PrefetchScalarGridSpec(
            num_scalar_prefetch=1,
            grid=(count // some,),
            in_specs=[
                at((some, height, width), base),
                at((some, height, width), 0),
                at((some, height, width), 0),
                at((some * width, columns), base),
                at((some, width, rank), base),
            ],
            out_specs=[
                at((some, 3 * height, columns), 0),
                at((some, rank, columns), 0),
            ],
        ),
        out_shape=[
            jax.ShapeDtypeStruct((count, 3 * height, columns), narrow),
            jax.ShapeDtypeStruct((count, rank, columns), wide),
        ],
        cost_estimate=pl.CostEstimate(
            flops=count * 2 * 3 * height * width * columns * 4,
            bytes_accessed=count * width * width * 2,
            transcendentals=0,
        ),
        compiler_params=pltpu.CompilerParams(vmem_limit_bytes=16 * 1024 * 1024),
    )(row, own, left, right, rhs, basis)


def far_leaves(row_ref, far_a, far_b, rhs, basis, coarse, part, vals, proj, lead):
    count = part.shape[0]
    height, width = far_a.shape[1], far_a.shape[2]
    half = count // 2
    at = turned(row_ref, 2, height)
    for k in range(count):
        rows = far_a[k] if k < half else far_b[k - half]
        got = narrow_dot(rows, rhs[k * width : (k + 1) * width, :]).astype(narrow)
        vals[k] = got
        total = part[k] + lax.dot_general(
            basis[k, pl.ds(at, height), :], got, FRONT, preferred_element_type=wide
        )
        proj[k] = total
        lead[k] = split_dot(coarse[k], total)


def far_body(*refs):
    far_leaves(*refs)


def last_body(
    row_ref, far_a, far_b, rhs, basis, coarse, part, ups, early, vals, proj, lead, late, up
):
    far_leaves(row_ref, far_a, far_b, rhs, basis, coarse, part, vals, proj, lead)
    slot = {12 + k: lead for k in range(4)}
    where = {12 + k: k for k in range(4)}
    for k, node in enumerate(EARLY):
        slot[16 + node], where[16 + node] = early, k
    for k, node in enumerate(LATE):
        pair = [slot[c][where[c]] for c in (2 * node, 2 * node + 1)]
        value = split_dot(ups[k], jnp.concatenate(pair, axis=0))
        if k == len(LATE) - 1:
            up[...] = value
        else:
            late[k] = value
        slot[16 + node], where[16 + node] = late, k


def far_shapes(count, height, rank, columns):
    return [
        jax.ShapeDtypeStruct((count, height, columns), narrow),
        jax.ShapeDtypeStruct((count, rank, columns), wide),
        jax.ShapeDtypeStruct((count, rank, columns), wide),
    ]


def merge_body(lead0, lead1, inv, basis, back, coarse, early, base):
    value = {}
    for k in range(4):
        value[k] = lead0[k]
    for k in range(8):
        value[4 + k] = lead1[k]
    for k, node in enumerate(EARLY):
        stacked = jnp.concatenate([value[2 * node], value[2 * node + 1]], axis=0)
        solved = split_dot(inv[node], stacked)
        reduced = split_dot(basis[node], solved, FRONT)
        value[16 + node] = split_dot(coarse[node], reduced)
        early[k] = value[16 + node]
        base[k] = solved - split_dot(back[node], reduced)


def prepare_body(inv, basis, back, coarse, ups, paths):
    for k, node in enumerate(LATE):
        ups[k] = split_dot(coarse[node], split_dot(basis[node], inv[node], FRONT))
    value = {30: None}
    rank = paths.shape[1]
    for node in reversed(range(15)):
        above = value[16 + node]
        below = back[node] if above is None else split_dot(back[node], above)
        for k in range(2):
            value[2 * node + k] = below[k * rank : (k + 1) * rank]
            if node < 8:
                paths[2 * node + k] = value[2 * node + k]


def known_body(lead2, late, early, base, inv, basis, back, proj0, proj1, proj2, rest):
    rank = proj0.shape[1]
    value = {12 + k: (lead2, k) for k in range(4)}
    for k, node in enumerate(EARLY):
        value[16 + node] = (early, k)
    for k, node in enumerate(LATE[:-1]):
        value[16 + node] = (late, k)
    known = {node: (lambda k=k: base[k]) for k, node in enumerate(EARLY)}
    for node in LATE:
        pair = [value[c][0][value[c][1]] for c in (2 * node, 2 * node + 1)]
        solved = split_dot(inv[node], jnp.concatenate(pair, axis=0))
        reduced = split_dot(basis[node], solved, FRONT)
        result = solved - split_dot(back[node], reduced)
        known[node] = lambda result=result: result
    projs = [(proj0, k) for k in range(4)] + [(proj1, k) for k in range(8)]
    projs += [(proj2, k) for k in range(4)]
    part = {30: None}
    for node in reversed(range(15)):
        halves = known[node]()
        if part[16 + node] is not None:
            halves = halves + split_dot(back[node], part[16 + node])
        for k in range(2):
            below = halves[k * rank : (k + 1) * rank]
            part[2 * node + k] = below
            if node < 8:
                ref, at = projs[2 * node + k]
                rest[2 * node + k] = ref[at] - below


def top_body(left_ref, packs, up_own, up_sib, down_own, down_sib):
    depth = down_own.shape[0]
    rank = packs.shape[0]
    path = None
    for level in range(depth):
        root = level == depth - 1
        first = 0 if root else 2 * rank + (depth - 2 - level) * 5 * rank
        is_left = left_ref[level] == 1

        def both(matrix):
            one, two = matrix[:, :rank], matrix[:, rank:]
            return jnp.where(is_left, one, two), jnp.where(is_left, two, one)

        if root:
            down = packs[:, first : first + 2 * rank]
        else:
            up_own[level], up_sib[level] = both(packs[:, first : first + 2 * rank])
            down = packs[:, first + 2 * rank : first + 4 * rank]
        if path is not None:
            down = split_dot(path, down)
        down_own[level], down_sib[level] = both(down)
        if not root:
            step = packs[:, first + 4 * rank : first + 5 * rank]
            path = step if path is None else split_dot(path, step)


def out_body(row_ref, top_ref, paths, rest, back, near0, near1, far, out):
    some, width = back.shape[0], back.shape[1]
    height = far.shape[1]
    top = top_ref[...]
    step = pl.program_id(0)
    at = [turned(row_ref, part, height) for part in (0, 3, 1, 2)]
    for k in range(some):
        difference = (rest[k] - split_dot(paths[k], top)).astype(narrow)
        matching = jnp.concatenate([back[k, pl.ds(a, height), :] for a in at], axis=0)
        change = narrow_dot(matching, difference)
        near = jnp.where(step == 0, near0[k], near1[k])
        for j, a in enumerate(at):
            block = far[k] if j == 3 else near[j * height : (j + 1) * height]
            out[pl.ds(pl.multiple_of(k * width + a, height), height), :] = (
                block.astype(wide) - change[j * height : (j + 1) * height]
            )


def out_call(row, top, paths, rest, back, near0, near1, far):
    leaves, width, rank = back.shape
    height, columns = far.shape[1], far.shape[2]
    some = near0.shape[0]

    def at(shape, index):
        return pl.BlockSpec(shape, lambda i, row: (index(i),) + (0,) * (len(shape) - 1))

    return pl.pallas_call(
        out_body,
        grid_spec=pltpu.PrefetchScalarGridSpec(
            num_scalar_prefetch=1,
            grid=(leaves // some,),
            in_specs=[
                pl.BlockSpec(top.shape, lambda i, row: (0, 0)),
                at((some, rank, rank), lambda i: i),
                at((some, rank, columns), lambda i: i),
                at((some, width, rank), lambda i: i),
                at((some, 3 * height, columns), lambda i: 0),
                at((some, 3 * height, columns), lambda i: jnp.maximum(i - 1, 0)),
                at((some, height, columns), lambda i: i),
            ],
            out_specs=at((some * width, columns), lambda i: i),
        ),
        out_shape=jax.ShapeDtypeStruct((leaves * width, columns), wide),
        compiler_params=pltpu.CompilerParams(vmem_limit_bytes=16 * 1024 * 1024),
        name="leaf_result",
    )(row, top, paths, rest, back, near0, near1, far)


def exact(eq, a, b):
    return jnp.einsum(eq, a, b, precision=lax.Precision.HIGHEST)


def top_factors(inv, basis, back, coarse, position, depth):
    total = lax.axis_size("leaf")
    rank = basis.shape[1]
    reduce_mat = exact("ik,ij->kj", basis, inv)
    up_mat = exact("kl,lj->kj", coarse, reduce_mat)
    down_mat = inv - exact("ik,kj->ij", back, reduce_mat)
    halves = [
        jnp.concatenate([up_mat, down_mat[s : s + rank], back[s : s + rank]], axis=1)
        for s in (0, rank)
    ]
    upper = None
    for bit in reversed(range(depth)):
        stride = 1 << bit
        high = (position >> bit) % 2 == 1
        if upper is None:
            got = lax.ppermute(inv[:rank], "leaf", [(stride, 0)])
            upper = jnp.where(high, inv[rank:], got)
            continue
        size, mine = upper.shape[1], halves[0].shape[1]
        most = max(size, mine)
        message = jnp.where(
            high,
            jnp.pad(halves[0], ((0, 0), (0, most - mine))),
            jnp.pad(upper, ((0, 0), (0, most - size))),
        )
        pairs = [(i, i ^ stride) for i in range(0, total, stride)]
        got = lax.ppermute(message, "leaf", pairs)
        upper = jnp.concatenate(
            [
                jnp.where(high, got[:, :size], upper),
                jnp.where(high, halves[1], got[:, :mine]),
            ],
            axis=1,
        )
    return upper


def solve(
    rhs_cols,
    leaf_inv,
    leaf_basis,
    leaf_back,
    leaf_coarse,
    mid_inv,
    mid_basis,
    mid_back,
    mid_coarse,
    top_inv,
    top_basis,
    top_back,
    top_coarse,
):
    leaf_count, height, width = leaf_inv.shape
    rank, columns = leaf_basis.shape[2], rhs_cols.shape[1]
    position = lax.axis_index("leaf")
    leaf_total = lax.axis_size("leaf")
    depth = leaf_total.bit_length() - 1
    ring = lax.axis_size("rhs")
    ahead = [(i, (i + 1) % ring) for i in range(ring)]
    behind = [(i, (i - 1) % ring) for i in range(ring)]
    cut = GROUPS[0][1]
    row = lax.axis_index("rhs").astype(jnp.int32).reshape(1)

    left, right = [], []
    for own in (leaf_inv[:cut], leaf_inv[cut:]):
        left.append(lax.ppermute(own, "rhs", ahead))
        right.append(lax.ppermute(own, "rhs", behind))
    far = []
    for k, (start, count) in enumerate(GROUPS):
        part = 0 if k == 0 else 1
        first = 0 if k == 0 else start - cut
        half = count // 2
        far.append(
            (
                lax.ppermute(left[part][first : first + half], "rhs", ahead),
                lax.ppermute(right[part][first + half : first + count], "rhs", behind),
            )
        )

    packs = top_factors(
        top_inv[0], top_basis[0], top_back[0], top_coarse[0], position, depth
    )
    sides = jnp.stack([1 - (position >> k) % 2 for k in range(depth)]).astype(jnp.int32)
    square = (rank, rank)
    up_own, up_sib, down_own, down_sib = kernel_call(
        top_body,
        [jax.ShapeDtypeStruct((n, *square), wide) for n in (depth - 1, depth - 1, depth, depth)],
        10**8,
        (sides, packs),
        scalars=1,
    )
    ups, paths = kernel_call(
        prepare_body,
        [
            jax.ShapeDtypeStruct((len(LATE), rank, 2 * rank), wide),
            jax.ShapeDtypeStruct((leaf_count, *square), wide),
        ],
        8 * 10**8,
        (mid_inv, mid_basis, mid_back, mid_coarse),
        room=24,
    )

    near0, part0 = near_call(0, row, leaf_inv, left[0], right[0], rhs_cols, leaf_basis)
    near1, part1 = near_call(cut, row, leaf_inv, left[1], right[1], rhs_cols, leaf_basis)

    def of_group(k):
        start, count = GROUPS[k]
        part = part0 if k == 0 else part1[start - cut : start - cut + count]
        return (
            row,
            *far[k],
            rhs_cols[start * width : (start + count) * width],
            leaf_basis[start : start + count],
            leaf_coarse[start : start + count],
            part,
        )

    results = [
        kernel_call(
            far_body,
            far_shapes(GROUPS[k][1], height, rank, columns),
            GROUPS[k][1] * 4 * 10**7,
            of_group(k),
            scalars=1,
        )
        for k in range(2)
    ]
    early, base = kernel_call(
        merge_body,
        [
            jax.ShapeDtypeStruct((len(EARLY), rank, columns), wide),
            jax.ShapeDtypeStruct((len(EARLY), 2 * rank, columns), wide),
        ],
        10**9,
        (results[0][2], results[1][2], mid_inv, mid_basis, mid_back, mid_coarse),
        room=24,
    )
    final = lax.optimization_barrier(
        (of_group(2), ups, early, up_own, up_sib, down_own, down_sib, paths)
    )
    group, ups, early, up_own, up_sib, down_own, down_sib, paths = final
    far2, proj2, lead2, late, current = kernel_call(
        last_body,
        far_shapes(GROUPS[2][1], height, rank, columns)
        + [
            jax.ShapeDtypeStruct((len(LATE) - 1, rank, columns), wide),
            jax.ShapeDtypeStruct((rank, columns), wide),
        ],
        3 * 10**8,
        (*group, ups, early),
        scalars=1,
    )
    rest = kernel_call(
        known_body,
        jax.ShapeDtypeStruct((leaf_count, rank, columns), wide),
        8 * 10**8,
        (
            lead2,
            late,
            early,
            base,
            mid_inv,
            mid_basis,
            mid_back,
            results[0][1],
            results[1][1],
            proj2,
        ),
        room=24,
    )
    far_vals = jnp.concatenate([results[0][0], results[1][0], far2], axis=0)

    top = None
    for level in range(depth):
        mask = 1 << level
        if level in (2, 4):
            mask |= mask >> 1
        pairs = [(i, i ^ mask) for i in range(leaf_total)]
        partner = lax.ppermute(current, "leaf", pairs)
        known = close_dot(down_own[level], current)
        top = known if top is None else top + known
        top = top + close_dot(down_sib[level], partner)
        if level < depth - 1:
            before = close_dot(up_own[level], current)
            current = before + close_dot(up_sib[level], partner)
    return out_call(row, top, paths, rest, leaf_back, near0, near1, far_vals)


def solution(mesh):
    return jax.shard_map(
        solve,
        mesh=mesh,
        in_specs=(P("leaf", "rhs"), P("leaf", "rhs", None))
        + (P("leaf", None, None),) * 11,
        out_specs=P("leaf", "rhs"),
        check_vma=False,
    )
```

```python
import functools

import jax
import jax.numpy as jnp
from jax import lax
from jax.experimental import pallas as pl
from jax.experimental.pallas import tpu as pltpu
from jax.sharding import PartitionSpec as P


wide = jnp.float32
narrow = jnp.bfloat16

GROUPS = ((0, 8), (8, 4), (12, 4))
PIECES = ((0, 4), (4, 4), (8, 8))
MERGED = ((0, 1, 2, 3, 8, 9, 12), (4, 5, 10))
LATE = (6, 7, 11, 13, 14)
FRONT = (((0,), (0,)), ((), ()))


def narrow_dot(a, b):
    return jnp.dot(a.astype(narrow), b.astype(narrow), preferred_element_type=wide)


def parts_of(a):
    high = a.astype(narrow)
    return high, (a - high.astype(wide)).astype(narrow)


def split_dot(a, b, dims=(((1,), (0,)), ((), ()))):
    a_high, a_low = parts_of(a)
    b_high, b_low = parts_of(b)

    def one(p, q):
        return lax.dot_general(p, q, dims, preferred_element_type=wide)

    return one(a_high, b_low) + one(a_low, b_high) + one(a_high, b_high)


def close_dot(a, b):
    return jnp.dot(a, b, precision=lax.Precision.HIGH, preferred_element_type=wide)


def kernel_call(body, out_shape, flops, operands, scalars=0, room=10, **more):
    if scalars:
        more["in_specs"] = [pl.BlockSpec(memory_space=pltpu.SMEM)] * scalars + [
            pl.BlockSpec(a.shape, lambda a=a: (0,) * a.ndim) for a in operands[scalars:]
        ]
    size = sum(a.size * a.dtype.itemsize for a in operands)
    return pl.pallas_call(
        body,
        out_shape=out_shape,
        cost_estimate=pl.CostEstimate(flops=flops, bytes_accessed=size, transcendentals=0),
        compiler_params=pltpu.CompilerParams(vmem_limit_bytes=room * 1024 * 1024),
        **more,
    )(*operands)


def turned(row_ref, part, height):
    return pl.multiple_of(lax.rem(row_ref[0] + part, 4) * height, height)


def near_body(row_ref, own, left, right, rhs, basis, vals, proj):
    count, height, width = own.shape
    for k in range(count):
        rows = jnp.concatenate([own[k], left[k], right[k]], axis=0)
        got = narrow_dot(rows, rhs[k * width : (k + 1) * width, :]).astype(narrow)
        vals[k] = got
        matching = jnp.concatenate(
            [basis[k, pl.ds(turned(row_ref, part, height), height), :] for part in (0, 3, 1)],
            axis=0,
        )
        proj[k] = lax.dot_general(matching, got, FRONT, preferred_element_type=wide)


def near_call(piece, row, own, left, right, rhs, basis):
    start, count = PIECES[piece]
    height, width = left.shape[1:]
    rank, columns = basis.shape[2], rhs.shape[1]
    some = 4
    base = start // some

    def at(shape, shift):
        return pl.BlockSpec(shape, lambda i, row: (shift + i,) + (0,) * (len(shape) - 1))

    return pl.pallas_call(
        near_body,
        grid_spec=pltpu.PrefetchScalarGridSpec(
            num_scalar_prefetch=1,
            grid=(count // some,),
            in_specs=[
                at((some, height, width), base),
                at((some, height, width), 0),
                at((some, height, width), 0),
                at((some * width, columns), base),
                at((some, width, rank), base),
            ],
            out_specs=[
                at((some, 3 * height, columns), 0),
                at((some, rank, columns), 0),
            ],
        ),
        out_shape=[
            jax.ShapeDtypeStruct((count, 3 * height, columns), narrow),
            jax.ShapeDtypeStruct((count, rank, columns), wide),
        ],
        cost_estimate=pl.CostEstimate(
            flops=count * 2 * 3 * height * width * columns * 4,
            bytes_accessed=count * width * width * 2,
            transcendentals=0,
        ),
        compiler_params=pltpu.CompilerParams(vmem_limit_bytes=8 * 1024 * 1024),
    )(row, own, left, right, rhs, basis)


def far_leaves(group, row_ref, far_a, far_b, rhs, basis, coarse, parts, vals, proj, lead):
    start, count = GROUPS[group]
    height, width = far_a.shape[1], far_a.shape[2]
    half = count // 2
    at = turned(row_ref, 2, height)
    for k in range(count):
        leaf = start + k
        rows = far_a[k] if k < half else far_b[k - half]
        got = narrow_dot(rows, rhs[leaf * width : (leaf + 1) * width, :]).astype(narrow)
        vals[k] = got
        before = parts[k // half][k % half] if group == 0 else parts[0][leaf - PIECES[2][0]]
        total = before + lax.dot_general(
            basis[leaf, pl.ds(at, height), :], got, FRONT, preferred_element_type=wide
        )
        proj[k] = total
        lead[k] = split_dot(coarse[leaf], total)


def far_body(group, refs):
    inputs, outputs = refs[:6], refs[-3:]
    far_leaves(group, *inputs, refs[6:-3], *outputs)


def last_body(
    row_ref, far_a, far_b, rhs, basis, coarse, part, ups, early0, early1,
    vals, proj, lead, late, up,
):
    far_leaves(2, row_ref, far_a, far_b, rhs, basis, coarse, (part,), vals, proj, lead)
    value = {12 + k: (lead, k) for k in range(4)}
    for early, nodes in zip((early0, early1), MERGED):
        for k, node in enumerate(nodes):
            value[16 + node] = (early, k)
    for k, node in enumerate(LATE):
        pair = [value[c][0][value[c][1]] for c in (2 * node, 2 * node + 1)]
        got = split_dot(ups[k], jnp.concatenate(pair, axis=0))
        if k == len(LATE) - 1:
            up[...] = got
        else:
            late[k] = got
        value[16 + node] = (late, k)


def far_shapes(count, height, rank, columns):
    return [
        jax.ShapeDtypeStruct((count, height, columns), narrow),
        jax.ShapeDtypeStruct((count, rank, columns), wide),
        jax.ShapeDtypeStruct((count, rank, columns), wide),
    ]


def merge_body(group, lead, inv, basis, back, coarse, early, base):
    value = {GROUPS[group][0] + k: (lead, k) for k in range(lead.shape[0])}
    for k, node in enumerate(MERGED[group]):
        pair = [value[c][0][value[c][1]] for c in (2 * node, 2 * node + 1)]
        solved = split_dot(inv[node], jnp.concatenate(pair, axis=0))
        reduced = split_dot(basis[node], solved, FRONT)
        early[k] = split_dot(coarse[node], reduced)
        base[k] = solved - split_dot(back[node], reduced)
        value[16 + node] = (early, k)


def prepare_body(inv, basis, back, coarse, ups, paths):
    for k, node in enumerate(LATE):
        ups[k] = split_dot(coarse[node], split_dot(basis[node], inv[node], FRONT))
    value = {30: None}
    rank = paths.shape[1]
    for node in reversed(range(15)):
        above = value[16 + node]
        below = back[node] if above is None else split_dot(back[node], above)
        for k in range(2):
            value[2 * node + k] = below[k * rank : (k + 1) * rank]
            if node < 8:
                paths[2 * node + k] = value[2 * node + k]


def late_body(lead2, late, early0, early1, inv, basis, back, base):
    value = {12 + k: (lead2, k) for k in range(4)}
    for early, nodes in zip((early0, early1), MERGED):
        for k, node in enumerate(nodes):
            value[16 + node] = (early, k)
    for k, node in enumerate(LATE[:-1]):
        value[16 + node] = (late, k)
    for k, node in enumerate(LATE):
        pair = [value[c][0][value[c][1]] for c in (2 * node, 2 * node + 1)]
        solved = split_dot(inv[node], jnp.concatenate(pair, axis=0))
        reduced = split_dot(basis[node], solved, FRONT)
        base[k] = solved - split_dot(back[node], reduced)


def known_body(base0, base1, base2, back, proj0, proj1, proj2, rest):
    rank = proj0.shape[1]
    known = {}
    for base, nodes in zip((base0, base1, base2), (*MERGED, LATE)):
        for k, node in enumerate(nodes):
            known[node] = (base, k)
    projs = [(proj, k) for proj in (proj0, proj1, proj2) for k in range(proj.shape[0])]
    part = {30: None}
    for node in reversed(range(15)):
        ref, at = known[node]
        halves = ref[at]
        if part[16 + node] is not None:
            halves = halves + split_dot(back[node], part[16 + node])
        for k in range(2):
            below = halves[k * rank : (k + 1) * rank]
            part[2 * node + k] = below
            if node < 8:
                ref, at = projs[2 * node + k]
                rest[2 * node + k] = ref[at] - below


def spread_body(size, flags, got, upper, low_half, high_half, wider, message):
    high, next_high = flags[0] == 1, flags[1] == 1
    mine = low_half.shape[1]
    if size:
        wider[:, :size] = jnp.where(high, got[:, :size], upper[...])
        wider[:, size:] = jnp.where(high, high_half[...], got[:, :mine])
    else:
        wider[...] = jnp.where(high, upper[...], got[...])
    held = wider.shape[1]
    both = min(mine, held)
    message[:, :both] = jnp.where(next_high, low_half[:, :both], wider[:, :both])
    if mine > held:
        message[:, held:] = low_half[:, held:]
    if held > mine:
        message[:, mine:] = wider[:, mine:]


def top_body(left_ref, got, upper, high_half, up_own, up_sib, down_own, down_sib, packs):
    depth = down_own.shape[0]
    rank = packs.shape[0]
    size = upper.shape[1]
    high = left_ref[0] == 0
    packs[:, :size] = jnp.where(high, got[:, :size], upper[...])
    packs[:, size:] = jnp.where(high, high_half[...], got[:, : high_half.shape[1]])
    path = None
    for level in range(depth):
        root = level == depth - 1
        first = 0 if root else 2 * rank + (depth - 2 - level) * 5 * rank
        is_left = left_ref[level] == 1

        def both(matrix):
            one, two = matrix[:, :rank], matrix[:, rank:]
            return jnp.where(is_left, one, two), jnp.where(is_left, two, one)

        if root:
            down = packs[:, first : first + 2 * rank]
        else:
            up_own[level], up_sib[level] = both(packs[:, first : first + 2 * rank])
            down = packs[:, first + 2 * rank : first + 4 * rank]
        if path is not None:
            down = split_dot(path, down)
        down_own[level], down_sib[level] = both(down)
        if not root:
            step = packs[:, first + 4 * rank : first + 5 * rank]
            path = step if path is None else split_dot(path, step)


def out_body(
    row_ref, top_ref, paths, rest, back, near0, near1, near2, far0, far1, far2, out
):
    some, width = back.shape[0], back.shape[1]
    height = far0.shape[1]
    top = top_ref[...]
    leaf = pl.program_id(0) * some
    at = [turned(row_ref, part, height) for part in (0, 3, 1, 2)]

    def pick(refs, spans, k):
        chosen = refs[-1][k]
        for ref, (start, _) in zip(refs[-2::-1], spans[:0:-1]):
            chosen = jnp.where(leaf < start, ref[k], chosen)
        return chosen

    for k in range(some):
        difference = (rest[k] - split_dot(paths[k], top)).astype(narrow)
        matching = jnp.concatenate([back[k, pl.ds(a, height), :] for a in at], axis=0)
        change = narrow_dot(matching, difference)
        near = pick((near0, near1, near2), PIECES, k)
        far = pick((far0, far1, far2), GROUPS, k)
        for j, a in enumerate(at):
            block = far if j == 3 else near[j * height : (j + 1) * height]
            out[pl.ds(pl.multiple_of(k * width + a, height), height), :] = (
                block.astype(wide) - change[j * height : (j + 1) * height]
            )


def out_call(row, top, paths, rest, back, nears, fars):
    leaves, width, rank = back.shape
    height, columns = fars[0].shape[1:]
    some = 2

    def at(shape):
        return pl.BlockSpec(shape, lambda i, row: (i,) + (0,) * (len(shape) - 1))

    def within(shape, span):
        first, most = span[0] // some, span[1] // some - 1
        return pl.BlockSpec(
            shape, lambda i, row: (jnp.clip(i - first, 0, most),) + (0,) * (len(shape) - 1)
        )

    return pl.pallas_call(
        out_body,
        grid_spec=pltpu.PrefetchScalarGridSpec(
            num_scalar_prefetch=1,
            grid=(leaves // some,),
            in_specs=[
                pl.BlockSpec(top.shape, lambda i, row: (0, 0)),
                at((some, rank, rank)),
                at((some, rank, columns)),
                at((some, width, rank)),
                *[within((some, 3 * height, columns), span) for span in PIECES],
                *[within((some, height, columns), span) for span in GROUPS],
            ],
            out_specs=at((some * width, columns)),
        ),
        out_shape=jax.ShapeDtypeStruct((leaves * width, columns), wide),
        compiler_params=pltpu.CompilerParams(vmem_limit_bytes=8 * 1024 * 1024),
        name="leaf_result",
    )(row, top, paths, rest, back, *nears, *fars)


def exact(eq, a, b):
    return jnp.einsum(eq, a, b, precision=lax.Precision.HIGHEST)


def top_factors(inv, basis, back, coarse, position, depth):
    total = lax.axis_size("leaf")
    rank = basis.shape[1]
    reduce_mat = exact("ik,ij->kj", basis, inv)
    up_mat = exact("kl,lj->kj", coarse, reduce_mat)
    down_mat = inv - exact("ik,kj->ij", back, reduce_mat)
    halves = [
        jnp.concatenate([up_mat, down_mat[s : s + rank], back[s : s + rank]], axis=1)
        for s in (0, rank)
    ]
    high = [((position >> bit) % 2).astype(jnp.int32) for bit in range(depth)]
    mine = halves[0].shape[1]
    upper, message, size = inv[rank:], inv[:rank], 0
    for bit in reversed(range(depth)):
        stride = 1 << bit
        if size == 0:
            pairs = [(stride, 0)]
        else:
            pairs = [(i, i ^ stride) for i in range(0, total, stride)]
        got = lax.ppermute(message, "leaf", pairs)
        if bit == 0:
            return got, upper, halves[1]
        held = size + mine if size else 2 * rank
        upper, message = kernel_call(
            functools.partial(spread_body, size),
            [
                jax.ShapeDtypeStruct((rank, held), wide),
                jax.ShapeDtypeStruct((rank, max(held, mine)), wide),
            ],
            10**6,
            (jnp.stack([high[bit], high[bit - 1]]), got, upper, *halves),
            scalars=1,
        )
        size = held


def solve(
    rhs_cols,
    leaf_inv,
    leaf_basis,
    leaf_back,
    leaf_coarse,
    mid_inv,
    mid_basis,
    mid_back,
    mid_coarse,
    top_inv,
    top_basis,
    top_back,
    top_coarse,
):
    leaf_count, height, _ = leaf_inv.shape
    rank, columns = leaf_basis.shape[2], rhs_cols.shape[1]
    position = lax.axis_index("leaf")
    leaf_total = lax.axis_size("leaf")
    depth = leaf_total.bit_length() - 1
    ring = lax.axis_size("rhs")
    ahead = [(i, (i + 1) % ring) for i in range(ring)]
    behind = [(i, (i - 1) % ring) for i in range(ring)]
    row = lax.axis_index("rhs").astype(jnp.int32).reshape(1)

    own = [leaf_inv[start : start + count] for start, count in PIECES]
    left, right = {}, {}
    for k, forth_first in ((0, True), (1, False), (1, True), (0, False), (2, True), (2, False)):
        if forth_first:
            left[k] = lax.ppermute(own[k], "rhs", ahead)
        else:
            right[k] = lax.ppermute(own[k], "rhs", behind)
    pairs = ((left[0], right[1]),) + tuple(
        (left[2][s : s + 2], right[2][s + 2 : s + 4]) for s in (0, 4)
    )
    far = [
        (lax.ppermute(one, "rhs", ahead), lax.ppermute(two, "rhs", behind))
        for one, two in pairs
    ]

    got, upper, own_half = top_factors(
        top_inv[0], top_basis[0], top_back[0], top_coarse[0], position, depth
    )
    sides = jnp.stack([1 - (position >> k) % 2 for k in range(depth)]).astype(jnp.int32)
    square = (rank, rank)
    up_own, up_sib, down_own, down_sib = kernel_call(
        top_body,
        [jax.ShapeDtypeStruct((n, *square), wide) for n in (depth - 1, depth - 1, depth, depth)],
        10**8,
        (sides, got, upper, own_half),
        scalars=1,
        scratch_shapes=[pltpu.VMEM((rank, upper.shape[1] + own_half.shape[1]), wide)],
    )
    ups, paths = kernel_call(
        prepare_body,
        [
            jax.ShapeDtypeStruct((len(LATE), rank, 2 * rank), wide),
            jax.ShapeDtypeStruct((leaf_count, *square), wide),
        ],
        8 * 10**8,
        (mid_inv, mid_basis, mid_back, mid_coarse),
        room=12,
    )

    nears, parts = [], []
    for k in range(len(PIECES)):
        near, part = near_call(k, row, leaf_inv, left[k], right[k], rhs_cols, leaf_basis)
        nears.append(near)
        parts.append(part)
    shared = (rhs_cols, leaf_basis, leaf_coarse)
    results, merged = [], []
    for k in range(2):
        count = GROUPS[k][1]
        results.append(
            kernel_call(
                lambda *refs, k=k: far_body(k, refs),
                far_shapes(count, height, rank, columns),
                count * 4 * 10**7,
                (row, *far[k], *shared, *(parts[:2] if k == 0 else parts[2:])),
                scalars=1,
            )
        )
        merged.append(
            kernel_call(
                functools.partial(merge_body, k),
                [
                    jax.ShapeDtypeStruct((len(MERGED[k]), rank, columns), wide),
                    jax.ShapeDtypeStruct((len(MERGED[k]), 2 * rank, columns), wide),
                ],
                len(MERGED[k]) * 10**8,
                (results[k][2], mid_inv, mid_basis, mid_back, mid_coarse),
                room=12,
            )
        )
    earlies = [m[0] for m in merged]
    final = lax.optimization_barrier(
        (far[2], parts[2], ups, earlies, up_own, up_sib, down_own, down_sib, paths)
    )
    last_far, part, ups, earlies, up_own, up_sib, down_own, down_sib, paths = final
    *last, late, current = kernel_call(
        last_body,
        far_shapes(GROUPS[2][1], height, rank, columns)
        + [
            jax.ShapeDtypeStruct((len(LATE) - 1, rank, columns), wide),
            jax.ShapeDtypeStruct((rank, columns), wide),
        ],
        3 * 10**8,
        (row, *last_far, *shared, part, ups, *earlies),
        scalars=1,
    )
    results.append(last)
    bases = [m[1] for m in merged]
    bases.append(
        kernel_call(
            late_body,
            jax.ShapeDtypeStruct((len(LATE), 2 * rank, columns), wide),
            4 * 10**8,
            (last[2], late, *earlies, mid_inv, mid_basis, mid_back),
            room=12,
        )
    )
    rest = kernel_call(
        known_body,
        jax.ShapeDtypeStruct((leaf_count, rank, columns), wide),
        4 * 10**8,
        (*bases, mid_back, *[r[1] for r in results]),
        room=12,
    )

    top = None
    for level in range(depth):
        mask = 1 << level
        if level in (2, 4):
            mask |= mask >> 1
        pairs = [(i, i ^ mask) for i in range(leaf_total)]
        partner = lax.ppermute(current, "leaf", pairs)
        known = close_dot(down_own[level], current)
        top = known if top is None else top + known
        top = top + close_dot(down_sib[level], partner)
        if level < depth - 1:
            before = close_dot(up_own[level], current)
            current = before + close_dot(up_sib[level], partner)
    return out_call(row, top, paths, rest, leaf_back, nears, [r[0] for r in results])


def solution(mesh):
    return jax.shard_map(
        solve,
        mesh=mesh,
        in_specs=(P("leaf", "rhs"), P("leaf", "rhs", None))
        + (P("leaf", None, None),) * 11,
        out_specs=P("leaf", "rhs"),
        check_vma=False,
    )
```

```python
import functools

import jax
import jax.numpy as jnp
from jax import lax
from jax.experimental import pallas as pl
from jax.experimental.pallas import tpu as pltpu
from jax.sharding import PartitionSpec as P


wide = jnp.float32
narrow = jnp.bfloat16

GROUPS = ((0, 8), (8, 8))
PIECES = ((0, 4), (4, 4), (8, 4), (12, 4))
MERGED = (0, 1, 2, 3, 8, 9, 12)
LATE = (4, 5, 6, 7, 10, 11, 13, 14)
FRONT = (((0,), (0,)), ((), ()))


def narrow_dot(a, b):
    return jnp.dot(a.astype(narrow), b.astype(narrow), preferred_element_type=wide)


def parts_of(a):
    high = a.astype(narrow)
    return high, (a - high.astype(wide)).astype(narrow)


def split_dot(a, b, dims=(((1,), (0,)), ((), ()))):
    rows_at = 1 - dims[0][0][0]
    left = jnp.concatenate(parts_of(a), axis=rows_at)
    right = jnp.concatenate(parts_of(b), axis=1)
    full = lax.dot_general(left, right, dims, preferred_element_type=wide)
    m, n = a.shape[rows_at], b.shape[1]
    return (full[m:, n:] + full[m:, :n] + full[:m, n:]) + full[:m, :n]


def close_dot(a, b):
    return jnp.dot(a, b, precision=lax.Precision.HIGH, preferred_element_type=wide)


def kernel_call(body, out_shape, flops, operands, scalars=0, room=10, **more):
    if scalars:
        more["in_specs"] = [pl.BlockSpec(memory_space=pltpu.SMEM)] * scalars + [
            pl.BlockSpec(a.shape, lambda a=a: (0,) * a.ndim) for a in operands[scalars:]
        ]
    size = sum(a.size * a.dtype.itemsize for a in operands)
    return pl.pallas_call(
        body,
        out_shape=out_shape,
        cost_estimate=pl.CostEstimate(flops=flops, bytes_accessed=size, transcendentals=0),
        compiler_params=pltpu.CompilerParams(vmem_limit_bytes=room * 1024 * 1024),
        **more,
    )(*operands)


def turned(row_ref, part, height):
    return pl.multiple_of(lax.rem(row_ref[0] + part, 4) * height, height)


def near_body(row_ref, own, left, right, rhs, basis, vals, proj):
    count, height, width = own.shape
    for k in range(count):
        rows = jnp.concatenate([own[k], left[k], right[k]], axis=0)
        got = narrow_dot(rows, rhs[k * width : (k + 1) * width, :])
        vals[k] = got.astype(narrow)
    at = [turned(row_ref, part, height) for part in (0, 3, 1)]
    for k in range(count):
        matching = jnp.concatenate([basis[k, pl.ds(a, height), :] for a in at], axis=0)
        proj[k] = lax.dot_general(matching, vals[k], FRONT, preferred_element_type=wide)


def near_call(piece, row, own, left, right, rhs, basis):
    start, count = PIECES[piece]
    height, width = left.shape[1:]
    rank, columns = basis.shape[2], rhs.shape[1]
    some = 4
    base = start // some

    def at(shape, shift):
        return pl.BlockSpec(shape, lambda i, row: (shift + i,) + (0,) * (len(shape) - 1))

    return pl.pallas_call(
        near_body,
        grid_spec=pltpu.PrefetchScalarGridSpec(
            num_scalar_prefetch=1,
            grid=(count // some,),
            in_specs=[
                at((some, height, width), base),
                at((some, height, width), 0),
                at((some, height, width), 0),
                at((some * width, columns), base),
                at((some, width, rank), base),
            ],
            out_specs=[
                at((some, 3 * height, columns), 0),
                at((some, rank, columns), 0),
            ],
        ),
        out_shape=[
            jax.ShapeDtypeStruct((count, 3 * height, columns), narrow),
            jax.ShapeDtypeStruct((count, rank, columns), wide),
        ],
        cost_estimate=pl.CostEstimate(
            flops=count * 2 * 3 * height * width * columns * 4,
            bytes_accessed=count * width * width * 2,
            transcendentals=0,
        ),
        compiler_params=pltpu.CompilerParams(vmem_limit_bytes=8 * 1024 * 1024),
    )(row, own, left, right, rhs, basis)


def far_leaves(
    group, row_ref, far_a, far_b, rhs, basis, coarse, part_a, part_b, vals, proj, lead
):
    start, count = GROUPS[group]
    height, width = far_a.shape[1], far_a.shape[2]
    half = count // 2
    at = turned(row_ref, 2, height)
    for k in range(count):
        leaf = start + k
        rows = far_a[k] if k < half else far_b[k - half]
        got = narrow_dot(rows, rhs[leaf * width : (leaf + 1) * width, :])
        vals[k] = got.astype(narrow)
    for k in range(count):
        before = part_a[k] if k < half else part_b[k - half]
        proj[k] = before + lax.dot_general(
            basis[start + k, pl.ds(at, height), :], vals[k], FRONT, preferred_element_type=wide
        )
    for k in range(count):
        lead[k] = split_dot(coarse[start + k], proj[k])


def last_body(
    row_ref, far_a, far_b, rhs, basis, coarse, part_a, part_b, ups, early,
    vals, proj, lead, late, up,
):
    far_leaves(
        1, row_ref, far_a, far_b, rhs, basis, coarse, part_a, part_b, vals, proj, lead
    )
    value = {8 + k: (lead, k) for k in range(8)}
    for k, node in enumerate(MERGED):
        value[16 + node] = (early, k)
    for k, node in enumerate(LATE):
        pair = [value[c][0][value[c][1]] for c in (2 * node, 2 * node + 1)]
        got = split_dot(ups[k], jnp.concatenate(pair, axis=0))
        if k == len(LATE) - 1:
            up[...] = got
        else:
            late[k] = got
        value[16 + node] = (late, k)


def far_shapes(count, height, rank, columns):
    return [
        jax.ShapeDtypeStruct((count, height, columns), narrow),
        jax.ShapeDtypeStruct((count, rank, columns), wide),
        jax.ShapeDtypeStruct((count, rank, columns), wide),
    ]


def by_level(nodes):
    for first, last in ((0, 8), (8, 12), (12, 14), (14, 15)):
        level = [(k, node) for k, node in enumerate(nodes) if first <= node < last]
        if level:
            yield level


def merge_body(lead, inv, basis, back, coarse, early, base):
    value = {k: (lead, k) for k in range(lead.shape[0])}
    for level in by_level(MERGED):
        solved, reduced = {}, {}
        for k, node in level:
            pair = [value[c][0][value[c][1]] for c in (2 * node, 2 * node + 1)]
            solved[k] = split_dot(inv[node], jnp.concatenate(pair, axis=0))
        for k, node in level:
            reduced[k] = split_dot(basis[node], solved[k], FRONT)
        for k, node in level:
            early[k] = split_dot(coarse[node], reduced[k])
            base[k] = solved[k] - split_dot(back[node], reduced[k])
            value[16 + node] = (early, k)


def prepare_body(inv, basis, back, coarse, ups, paths):
    for k, node in enumerate(LATE):
        ups[k] = split_dot(coarse[node], split_dot(basis[node], inv[node], FRONT))
    value = {30: None}
    rank = paths.shape[1]
    for node in reversed(range(15)):
        above = value[16 + node]
        below = back[node] if above is None else split_dot(back[node], above)
        for k in range(2):
            value[2 * node + k] = below[k * rank : (k + 1) * rank]
            if node < 8:
                paths[2 * node + k] = value[2 * node + k]


def late_body(lead, late, early, inv, basis, back, base):
    value = {8 + k: (lead, k) for k in range(8)}
    for k, node in enumerate(MERGED):
        value[16 + node] = (early, k)
    for k, node in enumerate(LATE[:-1]):
        value[16 + node] = (late, k)
    reduced = {}
    for k, node in enumerate(LATE):
        pair = [value[c][0][value[c][1]] for c in (2 * node, 2 * node + 1)]
        base[k] = split_dot(inv[node], jnp.concatenate(pair, axis=0))
    for k, node in enumerate(LATE):
        reduced[k] = split_dot(basis[node], base[k], FRONT)
    for k, node in enumerate(LATE):
        base[k] -= split_dot(back[node], reduced[k])


def known_body(base0, base1, back, proj0, proj1, rest):
    rank = proj0.shape[1]
    known = {}
    for base, nodes in ((base0, MERGED), (base1, LATE)):
        for k, node in enumerate(nodes):
            known[node] = (base, k)
    projs = [(proj, k) for proj in (proj0, proj1) for k in range(proj.shape[0])]
    part = {30: None}
    for node in reversed(range(15)):
        ref, at = known[node]
        halves = ref[at]
        if part[16 + node] is not None:
            halves = halves + split_dot(back[node], part[16 + node])
        for k in range(2):
            below = halves[k * rank : (k + 1) * rank]
            part[2 * node + k] = below
            if node < 8:
                ref, at = projs[2 * node + k]
                rest[2 * node + k] = ref[at] - below


def spread_body(size, flags, got, upper, low_half, high_half, wider, message):
    high, next_high = flags[0] == 1, flags[1] == 1
    mine = low_half.shape[1]
    if size:
        wider[:, :size] = jnp.where(high, got[:, :size], upper[...])
        wider[:, size:] = jnp.where(high, high_half[...], got[:, :mine])
    else:
        wider[...] = jnp.where(high, upper[...], got[...])
    held = wider.shape[1]
    both = min(mine, held)
    message[:, :both] = jnp.where(next_high, low_half[:, :both], wider[:, :both])
    if mine > held:
        message[:, held:] = low_half[:, held:]
    if held > mine:
        message[:, mine:] = wider[:, mine:]


def top_body(left_ref, got, upper, high_half, up_own, up_sib, down_own, down_sib, packs):
    depth = down_own.shape[0]
    rank = packs.shape[0]
    size = upper.shape[1]
    high = left_ref[0] == 0
    packs[:, :size] = jnp.where(high, got[:, :size], upper[...])
    packs[:, size:] = jnp.where(high, high_half[...], got[:, : high_half.shape[1]])
    path = None
    for level in range(depth):
        root = level == depth - 1
        first = 0 if root else 2 * rank + (depth - 2 - level) * 5 * rank
        is_left = left_ref[level] == 1

        def both(matrix):
            one, two = matrix[:, :rank], matrix[:, rank:]
            return jnp.where(is_left, one, two), jnp.where(is_left, two, one)

        if root:
            down = packs[:, first : first + 2 * rank]
        else:
            up_own[level], up_sib[level] = both(packs[:, first : first + 2 * rank])
            down = packs[:, first + 2 * rank : first + 4 * rank]
        if path is not None:
            down = split_dot(path, down)
        down_own[level], down_sib[level] = both(down)
        if not root:
            step = packs[:, first + 4 * rank : first + 5 * rank]
            path = step if path is None else split_dot(path, step)


def out_body(
    row_ref, top_ref, paths, rest, back, near0, near1, near2, near3, far0, far1, out
):
    some, width = back.shape[0], back.shape[1]
    height = far0.shape[1]
    top = top_ref[...]
    leaf = pl.program_id(0) * some
    at = [turned(row_ref, part, height) for part in (0, 3, 1, 2)]

    def pick(refs, spans, k):
        chosen = refs[-1][k]
        for ref, (start, _) in zip(refs[-2::-1], spans[:0:-1]):
            chosen = jnp.where(leaf < start, ref[k], chosen)
        return chosen

    for k in range(some):
        difference = (rest[k] - split_dot(paths[k], top)).astype(narrow)
        matching = jnp.concatenate([back[k, pl.ds(a, height), :] for a in at], axis=0)
        change = narrow_dot(matching, difference)
        near = pick((near0, near1, near2, near3), PIECES, k)
        far = pick((far0, far1), GROUPS, k)
        for j, a in enumerate(at):
            block = far if j == 3 else near[j * height : (j + 1) * height]
            out[pl.ds(pl.multiple_of(k * width + a, height), height), :] = (
                block.astype(wide) - change[j * height : (j + 1) * height]
            )


def out_call(row, top, paths, rest, back, nears, fars):
    leaves, width, rank = back.shape
    height, columns = fars[0].shape[1:]
    some = 4

    def at(shape):
        return pl.BlockSpec(shape, lambda i, row: (i,) + (0,) * (len(shape) - 1))

    def within(shape, span):
        first, most = span[0] // some, span[1] // some - 1
        return pl.BlockSpec(
            shape, lambda i, row: (jnp.clip(i - first, 0, most),) + (0,) * (len(shape) - 1)
        )

    return pl.pallas_call(
        out_body,
        grid_spec=pltpu.PrefetchScalarGridSpec(
            num_scalar_prefetch=1,
            grid=(leaves // some,),
            in_specs=[
                pl.BlockSpec(top.shape, lambda i, row: (0, 0)),
                at((some, rank, rank)),
                at((some, rank, columns)),
                at((some, width, rank)),
                *[within((some, 3 * height, columns), span) for span in PIECES],
                *[within((some, height, columns), span) for span in GROUPS],
            ],
            out_specs=at((some * width, columns)),
        ),
        out_shape=jax.ShapeDtypeStruct((leaves * width, columns), wide),
        compiler_params=pltpu.CompilerParams(vmem_limit_bytes=8 * 1024 * 1024),
        name="leaf_result",
    )(row, top, paths, rest, back, *nears, *fars)


def exact(eq, a, b):
    return jnp.einsum(eq, a, b, precision=lax.Precision.HIGHEST)


def top_factors(inv, basis, back, coarse, position, depth):
    total = lax.axis_size("leaf")
    rank = basis.shape[1]
    reduce_mat = exact("ik,ij->kj", basis, inv)
    up_mat = exact("kl,lj->kj", coarse, reduce_mat)
    down_mat = inv - exact("ik,kj->ij", back, reduce_mat)
    halves = [
        jnp.concatenate([up_mat, down_mat[s : s + rank], back[s : s + rank]], axis=1)
        for s in (0, rank)
    ]
    high = [((position >> bit) % 2).astype(jnp.int32) for bit in range(depth)]
    mine = halves[0].shape[1]
    upper, message, size = inv[rank:], inv[:rank], 0
    for bit in reversed(range(depth)):
        stride = 1 << bit
        if size == 0:
            pairs = [(stride, 0)]
        else:
            pairs = [(i, i ^ stride) for i in range(0, total, stride)]
        got = lax.ppermute(message, "leaf", pairs)
        if bit == 0:
            return got, upper, halves[1]
        held = size + mine if size else 2 * rank
        upper, message = kernel_call(
            functools.partial(spread_body, size),
            [
                jax.ShapeDtypeStruct((rank, held), wide),
                jax.ShapeDtypeStruct((rank, max(held, mine)), wide),
            ],
            10**6,
            (jnp.stack([high[bit], high[bit - 1]]), got, upper, *halves),
            scalars=1,
        )
        size = held


def solve(
    rhs_cols,
    leaf_inv,
    leaf_basis,
    leaf_back,
    leaf_coarse,
    mid_inv,
    mid_basis,
    mid_back,
    mid_coarse,
    top_inv,
    top_basis,
    top_back,
    top_coarse,
):
    leaf_count, height, _ = leaf_inv.shape
    rank, columns = leaf_basis.shape[2], rhs_cols.shape[1]
    position = lax.axis_index("leaf")
    leaf_total = lax.axis_size("leaf")
    depth = leaf_total.bit_length() - 1
    ring = lax.axis_size("rhs")
    ahead = [(i, (i + 1) % ring) for i in range(ring)]
    behind = [(i, (i - 1) % ring) for i in range(ring)]
    row = lax.axis_index("rhs").astype(jnp.int32).reshape(1)

    own, whole = [], leaf_inv
    for start, count in PIECES:
        own.append(whole[start : start + count])
        if start == 0:
            whole, own[0] = lax.optimization_barrier((whole, own[0]))
    left = [lax.ppermute(a, "rhs", ahead) for a in own]
    right = [lax.ppermute(a, "rhs", behind) for a in own]
    pairs = ((left[0], right[1]), (left[2], right[3]))
    far = [
        (lax.ppermute(one, "rhs", ahead), lax.ppermute(two, "rhs", behind))
        for one, two in pairs
    ]

    got, upper, own_half = top_factors(
        top_inv[0], top_basis[0], top_back[0], top_coarse[0], position, depth
    )
    sides = jnp.stack([1 - (position >> k) % 2 for k in range(depth)]).astype(jnp.int32)
    square = (rank, rank)
    up_own, up_sib, down_own, down_sib = kernel_call(
        top_body,
        [jax.ShapeDtypeStruct((n, *square), wide) for n in (depth - 1, depth - 1, depth, depth)],
        10**8,
        (sides, got, upper, own_half),
        scalars=1,
        scratch_shapes=[pltpu.VMEM((rank, upper.shape[1] + own_half.shape[1]), wide)],
    )
    ups, paths = kernel_call(
        prepare_body,
        [
            jax.ShapeDtypeStruct((len(LATE), rank, 2 * rank), wide),
            jax.ShapeDtypeStruct((leaf_count, *square), wide),
        ],
        8 * 10**8,
        (mid_inv, mid_basis, mid_back, mid_coarse),
        room=12,
    )

    nears, parts = [], []
    for k in range(len(PIECES)):
        near, part = near_call(k, row, leaf_inv, left[k], right[k], rhs_cols, leaf_basis)
        nears.append(near)
        parts.append(part)
    shared = (rhs_cols, leaf_basis, leaf_coarse)
    first = kernel_call(
        functools.partial(far_leaves, 0),
        far_shapes(GROUPS[0][1], height, rank, columns),
        3 * 10**8,
        (row, *far[0], *shared, *parts[:2]),
        scalars=1,
    )
    early, early_base = kernel_call(
        merge_body,
        [
            jax.ShapeDtypeStruct((len(MERGED), rank, columns), wide),
            jax.ShapeDtypeStruct((len(MERGED), 2 * rank, columns), wide),
        ],
        len(MERGED) * 10**8,
        (first[2], mid_inv, mid_basis, mid_back, mid_coarse),
        room=12,
    )
    final = lax.optimization_barrier(
        (far[1], parts[2:], ups, early, up_own, up_sib, down_own, down_sib, paths)
    )
    last_far, last_parts, ups, early, up_own, up_sib, down_own, down_sib, paths = final
    *last, late, current = kernel_call(
        last_body,
        far_shapes(GROUPS[1][1], height, rank, columns)
        + [
            jax.ShapeDtypeStruct((len(LATE) - 1, rank, columns), wide),
            jax.ShapeDtypeStruct((rank, columns), wide),
        ],
        4 * 10**8,
        (row, *last_far, *shared, *last_parts, ups, early),
        scalars=1,
    )
    late_base = kernel_call(
        late_body,
        jax.ShapeDtypeStruct((len(LATE), 2 * rank, columns), wide),
        6 * 10**8,
        (last[2], late, early, mid_inv, mid_basis, mid_back),
        room=12,
    )
    rest = kernel_call(
        known_body,
        jax.ShapeDtypeStruct((leaf_count, rank, columns), wide),
        4 * 10**8,
        (early_base, late_base, mid_back, first[1], last[1]),
        room=12,
    )

    top = None
    for level in range(depth):
        mask = 1 << level
        if level in (2, 4):
            mask |= mask >> 1
        pairs = [(i, i ^ mask) for i in range(leaf_total)]
        partner = lax.ppermute(current, "leaf", pairs)
        known = close_dot(down_own[level], current)
        top = known if top is None else top + known
        top = top + close_dot(down_sib[level], partner)
        if level < depth - 1:
            before = close_dot(up_own[level], current)
            current = before + close_dot(up_sib[level], partner)
    return out_call(row, top, paths, rest, leaf_back, nears, (first[0], last[0]))


def solution(mesh):
    return jax.shard_map(
        solve,
        mesh=mesh,
        in_specs=(P("leaf", "rhs"), P("leaf", "rhs", None))
        + (P("leaf", None, None),) * 11,
        out_specs=P("leaf", "rhs"),
        check_vma=False,
    )
```

```python
import functools

import jax
import jax.numpy as jnp
from jax import lax
from jax.experimental import pallas as pl
from jax.experimental.pallas import tpu as pltpu
from jax.sharding import PartitionSpec as P


wide = jnp.float32
narrow = jnp.bfloat16

GROUPS = ((0, 8), (8, 8))
PIECES = ((0, 4), (4, 4), (8, 4), (12, 4))
MERGED = (0, 1, 2, 3, 8, 9, 12)
LATE = (4, 5, 6, 7, 10, 11, 13, 14)
FRONT = (((0,), (0,)), ((), ()))


def narrow_dot(a, b):
    return jnp.dot(a.astype(narrow), b.astype(narrow), preferred_element_type=wide)


def parts_of(a):
    high = a.astype(narrow)
    return high, (a - high.astype(wide)).astype(narrow)


def split_dot(a, b, dims=(((1,), (0,)), ((), ()))):
    rows_at = 1 - dims[0][0][0]
    left = jnp.concatenate(parts_of(a), axis=rows_at)
    right = jnp.concatenate(parts_of(b), axis=1)
    full = lax.dot_general(left, right, dims, preferred_element_type=wide)
    m, n = a.shape[rows_at], b.shape[1]
    return (full[m:, n:] + full[m:, :n] + full[:m, n:]) + full[:m, :n]


def close_dot(a, b):
    return jnp.dot(a, b, precision=lax.Precision.HIGH, preferred_element_type=wide)


def kernel_call(body, out_shape, flops, operands, scalars=0, room=10, **more):
    if scalars:
        more["in_specs"] = [pl.BlockSpec(memory_space=pltpu.SMEM)] * scalars + [
            pl.BlockSpec(a.shape, lambda a=a: (0,) * a.ndim) for a in operands[scalars:]
        ]
    size = sum(a.size * a.dtype.itemsize for a in operands)
    return pl.pallas_call(
        body,
        out_shape=out_shape,
        cost_estimate=pl.CostEstimate(flops=flops, bytes_accessed=size, transcendentals=0),
        compiler_params=pltpu.CompilerParams(vmem_limit_bytes=room * 1024 * 1024),
        **more,
    )(*operands)


def turned(row_ref, part, height):
    return pl.multiple_of(lax.rem(row_ref[0] + part, 4) * height, height)


def near_body(row_ref, own, left, right, rhs, basis, vals, proj):
    count, height, width = own.shape
    for k in range(count):
        rows = jnp.concatenate([own[k], left[k], right[k]], axis=0)
        got = narrow_dot(rows, rhs[k * width : (k + 1) * width, :])
        vals[k] = got.astype(narrow)
    at = [turned(row_ref, part, height) for part in (0, 3, 1)]
    for k in range(count):
        matching = jnp.concatenate([basis[k, pl.ds(a, height), :] for a in at], axis=0)
        proj[k] = lax.dot_general(matching, vals[k], FRONT, preferred_element_type=wide)


def near_call(piece, row, own, left, right, rhs, basis):
    start, count = PIECES[piece]
    height, width = left.shape[1:]
    rank, columns = basis.shape[2], rhs.shape[1]
    some = 4
    base = start // some

    def at(shape, shift):
        return pl.BlockSpec(shape, lambda i, row: (shift + i,) + (0,) * (len(shape) - 1))

    return pl.pallas_call(
        near_body,
        grid_spec=pltpu.PrefetchScalarGridSpec(
            num_scalar_prefetch=1,
            grid=(count // some,),
            in_specs=[
                at((some, height, width), base),
                at((some, height, width), 0),
                at((some, height, width), 0),
                at((some * width, columns), base),
                at((some, width, rank), base),
            ],
            out_specs=[
                at((some, 3 * height, columns), 0),
                at((some, rank, columns), 0),
            ],
        ),
        out_shape=[
            jax.ShapeDtypeStruct((count, 3 * height, columns), narrow),
            jax.ShapeDtypeStruct((count, rank, columns), wide),
        ],
        cost_estimate=pl.CostEstimate(
            flops=count * 2 * 3 * height * width * columns * 4,
            bytes_accessed=count * width * width * 2,
            transcendentals=0,
        ),
        compiler_params=pltpu.CompilerParams(vmem_limit_bytes=8 * 1024 * 1024),
    )(row, own, left, right, rhs, basis)


def far_leaves(
    group, row_ref, far_a, far_b, rhs, basis, coarse, part_a, part_b, vals, proj, lead
):
    start, count = GROUPS[group]
    height, width = far_a.shape[1], far_a.shape[2]
    half = count // 2
    at = turned(row_ref, 2, height)
    for k in range(count):
        leaf = start + k
        rows = far_a[k] if k < half else far_b[k - half]
        got = narrow_dot(rows, rhs[leaf * width : (leaf + 1) * width, :])
        vals[k] = got.astype(narrow)
    for k in range(count):
        before = part_a[k] if k < half else part_b[k - half]
        proj[k] = before + lax.dot_general(
            basis[start + k, pl.ds(at, height), :], vals[k], FRONT, preferred_element_type=wide
        )
    for k in range(count):
        lead[k] = split_dot(coarse[start + k], proj[k])


def last_body(
    row_ref, far_a, far_b, rhs, basis, coarse, part_a, part_b, ups, early,
    vals, proj, lead, late, up,
):
    far_leaves(
        1, row_ref, far_a, far_b, rhs, basis, coarse, part_a, part_b, vals, proj, lead
    )
    value = {8 + k: (lead, k) for k in range(8)}
    for k, node in enumerate(MERGED):
        value[16 + node] = (early, k)
    for k, node in enumerate(LATE):
        pair = [value[c][0][value[c][1]] for c in (2 * node, 2 * node + 1)]
        got = split_dot(ups[k], jnp.concatenate(pair, axis=0))
        if k == len(LATE) - 1:
            up[...] = got
        else:
            late[k] = got
        value[16 + node] = (late, k)


def far_shapes(count, height, rank, columns):
    return [
        jax.ShapeDtypeStruct((count, height, columns), narrow),
        jax.ShapeDtypeStruct((count, rank, columns), wide),
        jax.ShapeDtypeStruct((count, rank, columns), wide),
    ]


def by_level(nodes):
    for first, last in ((0, 8), (8, 12), (12, 14), (14, 15)):
        level = [(k, node) for k, node in enumerate(nodes) if first <= node < last]
        if level:
            yield level


def merge_body(lead, inv, basis, back, coarse, early, base):
    value = {k: (lead, k) for k in range(lead.shape[0])}
    for level in by_level(MERGED):
        solved, reduced = {}, {}
        for k, node in level:
            pair = [value[c][0][value[c][1]] for c in (2 * node, 2 * node + 1)]
            solved[k] = split_dot(inv[node], jnp.concatenate(pair, axis=0))
        for k, node in level:
            reduced[k] = split_dot(basis[node], solved[k], FRONT)
        for k, node in level:
            early[k] = split_dot(coarse[node], reduced[k])
            base[k] = solved[k] - split_dot(back[node], reduced[k])
            value[16 + node] = (early, k)


def prepare_body(inv, basis, back, coarse, ups, paths):
    for k, node in enumerate(LATE):
        ups[k] = split_dot(coarse[node], split_dot(basis[node], inv[node], FRONT))
    value = {30: None}
    rank = paths.shape[1]
    for node in reversed(range(15)):
        above = value[16 + node]
        below = back[node] if above is None else split_dot(back[node], above)
        for k in range(2):
            value[2 * node + k] = below[k * rank : (k + 1) * rank]
            if node < 8:
                paths[2 * node + k] = value[2 * node + k]


def late_body(lead, late, early, inv, basis, back, base):
    value = {8 + k: (lead, k) for k in range(8)}
    for k, node in enumerate(MERGED):
        value[16 + node] = (early, k)
    for k, node in enumerate(LATE[:-1]):
        value[16 + node] = (late, k)
    reduced = {}
    for k, node in enumerate(LATE):
        pair = [value[c][0][value[c][1]] for c in (2 * node, 2 * node + 1)]
        base[k] = split_dot(inv[node], jnp.concatenate(pair, axis=0))
    for k, node in enumerate(LATE):
        reduced[k] = split_dot(basis[node], base[k], FRONT)
    for k, node in enumerate(LATE):
        base[k] -= split_dot(back[node], reduced[k])


def known_body(base0, base1, back, proj0, proj1, rest):
    rank = proj0.shape[1]
    known = {}
    for base, nodes in ((base0, MERGED), (base1, LATE)):
        for k, node in enumerate(nodes):
            known[node] = (base, k)
    projs = [(proj, k) for proj in (proj0, proj1) for k in range(proj.shape[0])]
    part = {30: None}
    for node in reversed(range(15)):
        ref, at = known[node]
        halves = ref[at]
        if part[16 + node] is not None:
            halves = halves + split_dot(back[node], part[16 + node])
        for k in range(2):
            below = halves[k * rank : (k + 1) * rank]
            part[2 * node + k] = below
            if node < 8:
                ref, at = projs[2 * node + k]
                rest[2 * node + k] = ref[at] - below


def spread_body(size, bit, spot, got, upper, low_half, high_half, wider, message):
    high, next_high = (lax.rem(spot[1] >> b, 2) == 1 for b in (bit, bit - 1))
    mine = low_half.shape[1]
    if size:
        wider[:, :size] = jnp.where(high, got[:, :size], upper[...])
        wider[:, size:] = jnp.where(high, high_half[...], got[:, :mine])
    else:
        wider[...] = jnp.where(high, upper[...], got[...])
    held = wider.shape[1]
    both = min(mine, held)
    message[:, :both] = jnp.where(next_high, low_half[:, :both], wider[:, :both])
    if mine > held:
        message[:, held:] = low_half[:, held:]
    if held > mine:
        message[:, mine:] = wider[:, mine:]


def top_body(spot, got, upper, high_half, up_own, up_sib, down_own, down_sib, packs):
    depth = down_own.shape[0]
    rank = packs.shape[0]
    size = upper.shape[1]
    high = lax.rem(spot[1], 2) == 1
    packs[:, :size] = jnp.where(high, got[:, :size], upper[...])
    packs[:, size:] = jnp.where(high, high_half[...], got[:, : high_half.shape[1]])
    path = None
    for level in range(depth):
        root = level == depth - 1
        first = 0 if root else 2 * rank + (depth - 2 - level) * 5 * rank
        is_left = lax.rem(spot[1] >> level, 2) == 0

        def both(matrix):
            one, two = matrix[:, :rank], matrix[:, rank:]
            return jnp.where(is_left, one, two), jnp.where(is_left, two, one)

        if root:
            down = packs[:, first : first + 2 * rank]
        else:
            up_own[level], up_sib[level] = both(packs[:, first : first + 2 * rank])
            down = packs[:, first + 2 * rank : first + 4 * rank]
        if path is not None:
            down = split_dot(path, down)
        down_own[level], down_sib[level] = both(down)
        if not root:
            step = packs[:, first + 4 * rank : first + 5 * rank]
            path = step if path is None else split_dot(path, step)


def out_body(
    row_ref, top_ref, paths, rest, back, near0, near1, near2, near3, far0, far1, out
):
    some, width = back.shape[0], back.shape[1]
    height = far0.shape[1]
    top = top_ref[...]
    leaf = pl.program_id(0) * some
    at = [turned(row_ref, part, height) for part in (0, 3, 1, 2)]

    def pick(refs, spans, k):
        chosen = refs[-1][k]
        for ref, (start, _) in zip(refs[-2::-1], spans[:0:-1]):
            chosen = jnp.where(leaf < start, ref[k], chosen)
        return chosen

    for k in range(some):
        difference = (rest[k] - split_dot(paths[k], top)).astype(narrow)
        matching = jnp.concatenate([back[k, pl.ds(a, height), :] for a in at], axis=0)
        change = narrow_dot(matching, difference)
        near = pick((near0, near1, near2, near3), PIECES, k)
        far = pick((far0, far1), GROUPS, k)
        for j, a in enumerate(at):
            block = far if j == 3 else near[j * height : (j + 1) * height]
            out[pl.ds(pl.multiple_of(k * width + a, height), height), :] = (
                block.astype(wide) - change[j * height : (j + 1) * height]
            )


def out_call(row, top, paths, rest, back, nears, fars):
    leaves, width, rank = back.shape
    height, columns = fars[0].shape[1:]
    some = 4

    def at(shape):
        return pl.BlockSpec(shape, lambda i, row: (i,) + (0,) * (len(shape) - 1))

    def within(shape, span):
        first, most = span[0] // some, span[1] // some - 1
        return pl.BlockSpec(
            shape, lambda i, row: (jnp.clip(i - first, 0, most),) + (0,) * (len(shape) - 1)
        )

    return pl.pallas_call(
        out_body,
        grid_spec=pltpu.PrefetchScalarGridSpec(
            num_scalar_prefetch=1,
            grid=(leaves // some,),
            in_specs=[
                pl.BlockSpec(top.shape, lambda i, row: (0, 0)),
                at((some, rank, rank)),
                at((some, rank, columns)),
                at((some, width, rank)),
                *[within((some, 3 * height, columns), span) for span in PIECES],
                *[within((some, height, columns), span) for span in GROUPS],
            ],
            out_specs=at((some * width, columns)),
        ),
        out_shape=jax.ShapeDtypeStruct((leaves * width, columns), wide),
        compiler_params=pltpu.CompilerParams(vmem_limit_bytes=8 * 1024 * 1024),
        name="leaf_result",
    )(row, top, paths, rest, back, *nears, *fars)


def exact(eq, a, b):
    return jnp.einsum(eq, a, b, precision=lax.Precision.HIGHEST)


def top_factors(inv, basis, back, coarse, spot, depth):
    total = lax.axis_size("leaf")
    rank = basis.shape[1]
    reduce_mat = exact("ik,ij->kj", basis, inv)
    up_mat = exact("kl,lj->kj", coarse, reduce_mat)
    down_mat = inv - exact("ik,kj->ij", back, reduce_mat)
    halves = [
        jnp.concatenate([up_mat, down_mat[s : s + rank], back[s : s + rank]], axis=1)
        for s in (0, rank)
    ]
    mine = halves[0].shape[1]
    upper, message, size = inv[rank:], inv[:rank], 0
    for bit in reversed(range(depth)):
        stride = 1 << bit
        if size == 0:
            pairs = [(stride, 0)]
        else:
            pairs = [(i, i ^ stride) for i in range(0, total, stride)]
        got = lax.ppermute(message, "leaf", pairs)
        if bit == 0:
            return got, upper, halves[1]
        held = size + mine if size else 2 * rank
        upper, message = kernel_call(
            functools.partial(spread_body, size, bit),
            [
                jax.ShapeDtypeStruct((rank, held), wide),
                jax.ShapeDtypeStruct((rank, max(held, mine)), wide),
            ],
            10**6,
            (spot, got, upper, *halves),
            scalars=1,
        )
        size = held


def solve(
    rhs_cols,
    leaf_inv,
    leaf_basis,
    leaf_back,
    leaf_coarse,
    mid_inv,
    mid_basis,
    mid_back,
    mid_coarse,
    top_inv,
    top_basis,
    top_back,
    top_coarse,
):
    leaf_count, height, _ = leaf_inv.shape
    rank, columns = leaf_basis.shape[2], rhs_cols.shape[1]
    position = lax.axis_index("leaf")
    leaf_total = lax.axis_size("leaf")
    depth = leaf_total.bit_length() - 1
    ring = lax.axis_size("rhs")
    ahead = [(i, (i + 1) % ring) for i in range(ring)]
    behind = [(i, (i - 1) % ring) for i in range(ring)]
    row = jnp.stack([lax.axis_index("rhs"), position]).astype(jnp.int32)

    own, whole = [], leaf_inv
    for start, count in PIECES:
        own.append(whole[start : start + count])
        if start == 0:
            whole, own[0], row = lax.optimization_barrier((whole, own[0], row))
    left = [lax.ppermute(a, "rhs", ahead) for a in own]
    right = [lax.ppermute(a, "rhs", behind) for a in own]
    pairs = ((left[0], right[1]), (left[2], right[3]))
    far = [
        (lax.ppermute(one, "rhs", ahead), lax.ppermute(two, "rhs", behind))
        for one, two in pairs
    ]

    got, upper, own_half = top_factors(
        top_inv[0], top_basis[0], top_back[0], top_coarse[0], row, depth
    )
    square = (rank, rank)
    up_own, up_sib, down_own, down_sib = kernel_call(
        top_body,
        [jax.ShapeDtypeStruct((n, *square), wide) for n in (depth - 1, depth - 1, depth, depth)],
        10**8,
        (row, got, upper, own_half),
        scalars=1,
        scratch_shapes=[pltpu.VMEM((rank, upper.shape[1] + own_half.shape[1]), wide)],
    )
    ups, paths = kernel_call(
        prepare_body,
        [
            jax.ShapeDtypeStruct((len(LATE), rank, 2 * rank), wide),
            jax.ShapeDtypeStruct((leaf_count, *square), wide),
        ],
        8 * 10**8,
        (mid_inv, mid_basis, mid_back, mid_coarse),
        room=12,
    )

    nears, parts = [], []
    for k in range(len(PIECES)):
        near, part = near_call(k, row, leaf_inv, left[k], right[k], rhs_cols, leaf_basis)
        nears.append(near)
        parts.append(part)
    shared = (rhs_cols, leaf_basis, leaf_coarse)
    first = kernel_call(
        functools.partial(far_leaves, 0),
        far_shapes(GROUPS[0][1], height, rank, columns),
        3 * 10**8,
        (row, *far[0], *shared, *parts[:2]),
        scalars=1,
    )
    early, early_base = kernel_call(
        merge_body,
        [
            jax.ShapeDtypeStruct((len(MERGED), rank, columns), wide),
            jax.ShapeDtypeStruct((len(MERGED), 2 * rank, columns), wide),
        ],
        len(MERGED) * 10**8,
        (first[2], mid_inv, mid_basis, mid_back, mid_coarse),
        room=12,
    )
    final = lax.optimization_barrier(
        (far[1], parts[2:], ups, early, up_own, up_sib, down_own, down_sib, paths)
    )
    last_far, last_parts, ups, early, up_own, up_sib, down_own, down_sib, paths = final
    *last, late, current = kernel_call(
        last_body,
        far_shapes(GROUPS[1][1], height, rank, columns)
        + [
            jax.ShapeDtypeStruct((len(LATE) - 1, rank, columns), wide),
            jax.ShapeDtypeStruct((rank, columns), wide),
        ],
        4 * 10**8,
        (row, *last_far, *shared, *last_parts, ups, early),
        scalars=1,
    )
    late_base = kernel_call(
        late_body,
        jax.ShapeDtypeStruct((len(LATE), 2 * rank, columns), wide),
        6 * 10**8,
        (last[2], late, early, mid_inv, mid_basis, mid_back),
        room=12,
    )
    rest = kernel_call(
        known_body,
        jax.ShapeDtypeStruct((leaf_count, rank, columns), wide),
        4 * 10**8,
        (early_base, late_base, mid_back, first[1], last[1]),
        room=12,
    )

    top = None
    for level in range(depth):
        mask = 1 << level
        if level in (2, 4):
            mask |= mask >> 1
        pairs = [(i, i ^ mask) for i in range(leaf_total)]
        partner = lax.ppermute(current, "leaf", pairs)
        known = close_dot(down_own[level], current)
        top = known if top is None else top + known
        top = top + close_dot(down_sib[level], partner)
        if level < depth - 1:
            before = close_dot(up_own[level], current)
            current = before + close_dot(up_sib[level], partner)
    return out_call(row, top, paths, rest, leaf_back, nears, (first[0], last[0]))


def solution(mesh):
    return jax.shard_map(
        solve,
        mesh=mesh,
        in_specs=(P("leaf", "rhs"), P("leaf", "rhs", None))
        + (P("leaf", None, None),) * 11,
        out_specs=P("leaf", "rhs"),
        check_vma=False,
    )
```

```python
import functools

import jax
import jax.numpy as jnp
from jax import lax
from jax.experimental import pallas as pl
from jax.experimental.pallas import tpu as pltpu
from jax.sharding import PartitionSpec as P


wide = jnp.float32
narrow = jnp.bfloat16

GROUPS = ((0, 8), (8, 8))
PIECES = ((0, 4), (4, 4), (8, 4), (12, 4))
MERGED = (0, 1, 2, 3, 8, 9, 12)
LATE = (4, 5, 6, 7, 10, 11, 13, 14)
FRONT = (((0,), (0,)), ((), ()))


def narrow_dot(a, b):
    return jnp.dot(a.astype(narrow), b.astype(narrow), preferred_element_type=wide)


def parts_of(a):
    high = a.astype(narrow)
    return high, (a - high.astype(wide)).astype(narrow)


def split_dot(a, b, dims=(((1,), (0,)), ((), ()))):
    rows_at = 1 - dims[0][0][0]
    left = jnp.concatenate(parts_of(a), axis=rows_at)
    right = jnp.concatenate(parts_of(b), axis=1)
    full = lax.dot_general(left, right, dims, preferred_element_type=wide)
    m, n = a.shape[rows_at], b.shape[1]
    return (full[m:, n:] + full[m:, :n] + full[:m, n:]) + full[:m, :n]


def kernel_call(body, out_shape, flops, operands, scalars=0, room=10, **more):
    if scalars:
        more["in_specs"] = [pl.BlockSpec(memory_space=pltpu.SMEM)] * scalars + [
            pl.BlockSpec(a.shape, lambda a=a: (0,) * a.ndim) for a in operands[scalars:]
        ]
    size = sum(a.size * a.dtype.itemsize for a in operands)
    return pl.pallas_call(
        body,
        out_shape=out_shape,
        cost_estimate=pl.CostEstimate(flops=flops, bytes_accessed=size, transcendentals=0),
        compiler_params=pltpu.CompilerParams(vmem_limit_bytes=room * 1024 * 1024),
        **more,
    )(*operands)


def turned(row_ref, part, height):
    return pl.multiple_of(lax.rem(row_ref[0] + part, 4) * height, height)


def near_body(row_ref, own, left, right, rhs, basis, vals, proj):
    count, height, width = own.shape
    for k in range(count):
        rows = jnp.concatenate([own[k], left[k], right[k]], axis=0)
        got = narrow_dot(rows, rhs[k * width : (k + 1) * width, :])
        vals[k] = got.astype(narrow)
    at = [turned(row_ref, part, height) for part in (0, 3, 1)]
    for k in range(count):
        matching = jnp.concatenate([basis[k, pl.ds(a, height), :] for a in at], axis=0)
        proj[k] = lax.dot_general(matching, vals[k], FRONT, preferred_element_type=wide)


def near_call(piece, row, own, left, right, rhs, basis):
    start, count = PIECES[piece]
    height, width = left.shape[1:]
    rank, columns = basis.shape[2], rhs.shape[1]
    some = 4
    base = start // some

    def at(shape, shift):
        return pl.BlockSpec(shape, lambda i, row: (shift + i,) + (0,) * (len(shape) - 1))

    return pl.pallas_call(
        near_body,
        grid_spec=pltpu.PrefetchScalarGridSpec(
            num_scalar_prefetch=1,
            grid=(count // some,),
            in_specs=[
                at((some, height, width), base),
                at((some, height, width), 0),
                at((some, height, width), 0),
                at((some * width, columns), base),
                at((some, width, rank), base),
            ],
            out_specs=[
                at((some, 3 * height, columns), 0),
                at((some, rank, columns), 0),
            ],
        ),
        out_shape=[
            jax.ShapeDtypeStruct((count, 3 * height, columns), narrow),
            jax.ShapeDtypeStruct((count, rank, columns), wide),
        ],
        cost_estimate=pl.CostEstimate(
            flops=count * 2 * 3 * height * width * columns * 4,
            bytes_accessed=count * width * width * 2,
            transcendentals=0,
        ),
        compiler_params=pltpu.CompilerParams(vmem_limit_bytes=8 * 1024 * 1024),
    )(row, own, left, right, rhs, basis)


def far_leaves(
    group, row_ref, far_a, far_b, rhs, basis, coarse, part_a, part_b, vals, proj, lead
):
    start, count = GROUPS[group]
    height, width = far_a.shape[1], far_a.shape[2]
    half = count // 2
    at = turned(row_ref, 2, height)
    for k in range(count):
        leaf = start + k
        rows = far_a[k] if k < half else far_b[k - half]
        got = narrow_dot(rows, rhs[leaf * width : (leaf + 1) * width, :])
        vals[k] = got.astype(narrow)
    for k in range(count):
        before = part_a[k] if k < half else part_b[k - half]
        proj[k] = before + lax.dot_general(
            basis[start + k, pl.ds(at, height), :], vals[k], FRONT, preferred_element_type=wide
        )
    for k in range(count):
        lead[k] = split_dot(coarse[start + k], proj[k])


def last_body(
    row_ref, far_a, far_b, rhs, basis, coarse, part_a, part_b, ups, early,
    vals, proj, lead, late, up,
):
    far_leaves(
        1, row_ref, far_a, far_b, rhs, basis, coarse, part_a, part_b, vals, proj, lead
    )
    value = {8 + k: (lead, k) for k in range(8)}
    for k, node in enumerate(MERGED):
        value[16 + node] = (early, k)
    for k, node in enumerate(LATE):
        pair = [value[c][0][value[c][1]] for c in (2 * node, 2 * node + 1)]
        got = split_dot(ups[k], jnp.concatenate(pair, axis=0))
        if k == len(LATE) - 1:
            up[...] = got
        else:
            late[k] = got
        value[16 + node] = (late, k)


def far_shapes(count, height, rank, columns):
    return [
        jax.ShapeDtypeStruct((count, height, columns), narrow),
        jax.ShapeDtypeStruct((count, rank, columns), wide),
        jax.ShapeDtypeStruct((count, rank, columns), wide),
    ]


def by_level(nodes):
    for first, last in ((0, 8), (8, 12), (12, 14), (14, 15)):
        level = [(k, node) for k, node in enumerate(nodes) if first <= node < last]
        if level:
            yield level


def merge_body(lead, inv, basis, back, coarse, early, base):
    value = {k: (lead, k) for k in range(lead.shape[0])}
    for level in by_level(MERGED):
        solved, reduced = {}, {}
        for k, node in level:
            pair = [value[c][0][value[c][1]] for c in (2 * node, 2 * node + 1)]
            solved[k] = split_dot(inv[node], jnp.concatenate(pair, axis=0))
        for k, node in level:
            reduced[k] = split_dot(basis[node], solved[k], FRONT)
        for k, node in level:
            early[k] = split_dot(coarse[node], reduced[k])
            base[k] = solved[k] - split_dot(back[node], reduced[k])
            value[16 + node] = (early, k)


def prepare_body(inv, basis, back, coarse, ups, paths):
    for k, node in enumerate(LATE):
        ups[k] = split_dot(coarse[node], split_dot(basis[node], inv[node], FRONT))
    value = {30: None}
    rank = paths.shape[1]
    for node in reversed(range(15)):
        above = value[16 + node]
        below = back[node] if above is None else split_dot(back[node], above)
        for k in range(2):
            value[2 * node + k] = below[k * rank : (k + 1) * rank]
            if node < 8:
                paths[2 * node + k] = value[2 * node + k]


def late_body(lead, late, early, inv, basis, back, base):
    value = {8 + k: (lead, k) for k in range(8)}
    for k, node in enumerate(MERGED):
        value[16 + node] = (early, k)
    for k, node in enumerate(LATE[:-1]):
        value[16 + node] = (late, k)
    reduced = {}
    for k, node in enumerate(LATE):
        pair = [value[c][0][value[c][1]] for c in (2 * node, 2 * node + 1)]
        base[k] = split_dot(inv[node], jnp.concatenate(pair, axis=0))
    for k, node in enumerate(LATE):
        reduced[k] = split_dot(basis[node], base[k], FRONT)
    for k, node in enumerate(LATE):
        base[k] -= split_dot(back[node], reduced[k])


def known_body(base0, base1, back, proj0, proj1, rest):
    rank = proj0.shape[1]
    known = {}
    for base, nodes in ((base0, MERGED), (base1, LATE)):
        for k, node in enumerate(nodes):
            known[node] = (base, k)
    projs = [(proj, k) for proj in (proj0, proj1) for k in range(proj.shape[0])]
    part = {30: None}
    for node in reversed(range(15)):
        ref, at = known[node]
        halves = ref[at]
        if part[16 + node] is not None:
            halves = halves + split_dot(back[node], part[16 + node])
        for k in range(2):
            below = halves[k * rank : (k + 1) * rank]
            part[2 * node + k] = below
            if node < 8:
                ref, at = projs[2 * node + k]
                rest[2 * node + k] = ref[at] - below


def spread_body(size, mine, next_mine, bit, spot, got, upper, low_half, high_half, wider, message):
    high, next_high = (lax.rem(spot[1] >> b, 2) == 1 for b in (bit, bit - 1))
    if size:
        wider[:, :size] = jnp.where(high, got[:, :size], upper[...])
        wider[:, size:] = jnp.where(high, high_half[:, :mine], got[:, :mine])
    else:
        wider[...] = jnp.where(high, upper[...], got[...])
    held = wider.shape[1]
    both = min(next_mine, held)
    message[:, :both] = jnp.where(next_high, low_half[:, :both], wider[:, :both])
    if next_mine > held:
        message[:, held:] = low_half[:, held:next_mine]
    if held > next_mine:
        message[:, next_mine:] = wider[:, next_mine:]


def top_body(spot, got, upper, high_half, up_first, down_first, up_x, down_x, down_y, packs):
    rank = packs.shape[0]
    size = upper.shape[1]
    mine = pack_width(0, rank)
    high = lax.rem(spot[1], 2) == 1
    packs[:, :size] = jnp.where(high, got[:, :size], upper[...])
    packs[:, size:] = jnp.where(high, high_half[:, :mine], got[:, :mine])

    def sided(level, matrix):
        is_left = lax.rem(spot[1] >> level, 2) == 0
        one, two = matrix[:, :rank], matrix[:, rank:]
        return jnp.concatenate(
            [jnp.where(is_left, one, two), jnp.where(is_left, two, one)], axis=1
        )

    ups, downs, sibling, path = {}, {}, {}, None
    end = packs.shape[1]
    for level in range(4):
        first = end - pack_width(level, rank)
        end = first
        ups[level] = sided(level, packs[:, first : first + 2 * rank])
        down = packs[:, first + 2 * rank : first + 4 * rank]
        downs[level] = sided(level, down if path is None else split_dot(path, down))
        step = packs[:, first + 4 * rank : first + 5 * rank]
        path = step if path is None else split_dot(path, step)
        if level % 2:
            sibling[level] = sided(level, packs[:, first + 5 * rank : first + 7 * rank])
    downs[4] = sided(4, split_dot(path, packs[:, : 2 * rank]))

    def joined(above, low):
        near = split_dot(above[:, :rank], ups[low])
        return near, split_dot(above[:, rank:], sibling[low])

    up_first[...] = ups[0]
    down_first[...] = downs[0]
    up_x[:, : 2 * rank], up_x[:, 2 * rank :] = joined(ups[2], 1)
    for out, low in ((down_x, 1), (down_y, 3)):
        near, away = joined(downs[low + 1], low)
        out[:, : 2 * rank] = downs[low] + near
        out[:, 2 * rank :] = away


def join_body(matrix, *refs):
    refs[-1][...] = split_dot(
        matrix[...], jnp.concatenate([r[...] for r in refs[:-1]], axis=0)
    )


def below_body(first, second, *refs):
    out = refs[-1]
    out[...] = split_dot(
        first[...], jnp.concatenate([r[...] for r in refs[:2]], axis=0)
    ) + split_dot(second[...], jnp.concatenate([r[...] for r in refs[2:-1]], axis=0))


def end_body(matrix, before, *refs):
    refs[-1][...] = before[...] + split_dot(
        matrix[...], jnp.concatenate([r[...] for r in refs[:-1]], axis=0)
    )


def pack_width(bit, rank):
    return (7 if bit % 2 else 5) * rank


def out_body(
    row_ref, top_ref, paths, rest, back, near0, near1, near2, near3, far0, far1, out
):
    some, width = back.shape[0], back.shape[1]
    height = far0.shape[1]
    top = top_ref[...]
    at = [turned(row_ref, part, height) for part in (0, 3, 1, 2)]

    def leaves_of(near, far):
        for k in range(some):
            difference = (rest[k] - split_dot(paths[k], top)).astype(narrow)
            matching = jnp.concatenate([back[k, pl.ds(a, height), :] for a in at], axis=0)
            change = narrow_dot(matching, difference)
            for j, a in enumerate(at):
                block = far[k] if j == 3 else near[k, j * height : (j + 1) * height, :]
                out[pl.ds(pl.multiple_of(k * width + a, height), height), :] = (
                    block.astype(wide) - change[j * height : (j + 1) * height]
                )

    for step, near in enumerate((near0, near1, near2, near3)):
        far = (far0, far1)[step // 2]

        @pl.when(pl.program_id(0) == step)
        def _(near=near, far=far):
            leaves_of(near, far)


def out_call(row, top, paths, rest, back, nears, fars):
    leaves, width, rank = back.shape
    height, columns = fars[0].shape[1:]
    some = 4

    def at(shape):
        return pl.BlockSpec(shape, lambda i, row: (i,) + (0,) * (len(shape) - 1))

    def within(shape, span):
        first, most = span[0] // some, span[1] // some - 1
        return pl.BlockSpec(
            shape, lambda i, row: (jnp.clip(i - first, 0, most),) + (0,) * (len(shape) - 1)
        )

    return pl.pallas_call(
        out_body,
        grid_spec=pltpu.PrefetchScalarGridSpec(
            num_scalar_prefetch=1,
            grid=(leaves // some,),
            in_specs=[
                pl.BlockSpec(top.shape, lambda i, row: (0, 0)),
                at((some, rank, rank)),
                at((some, rank, columns)),
                at((some, width, rank)),
                *[within((some, 3 * height, columns), span) for span in PIECES],
                *[within((some, height, columns), span) for span in GROUPS],
            ],
            out_specs=at((some * width, columns)),
        ),
        out_shape=jax.ShapeDtypeStruct((leaves * width, columns), wide),
        compiler_params=pltpu.CompilerParams(vmem_limit_bytes=8 * 1024 * 1024),
        name="leaf_result",
    )(row, top, paths, rest, back, *nears, *fars)


def exact(eq, a, b):
    return jnp.einsum(eq, a, b, precision=lax.Precision.HIGHEST)


def top_factors(inv, basis, back, coarse, spot, depth):
    total = lax.axis_size("leaf")
    rank = basis.shape[1]
    reduce_mat = exact("ik,ij->kj", basis, inv)
    up_mat = exact("kl,lj->kj", coarse, reduce_mat)
    down_mat = inv - exact("ik,kj->ij", back, reduce_mat)
    swaps = [
        (i, i ^ (2 * stride)) for stride in (2, 8) for i in range(stride, total, 2 * stride)
    ]
    swapped = lax.ppermute(up_mat, "leaf", swaps)
    halves = [
        jnp.concatenate([up_mat, down_mat[s : s + rank], back[s : s + rank], swapped], axis=1)
        for s in (0, rank)
    ]
    upper, message, size = inv[rank:], inv[:rank], 0
    for bit in reversed(range(depth)):
        stride = 1 << bit
        if size == 0:
            pairs = [(stride, 0)]
        else:
            pairs = [(i, i ^ stride) for i in range(0, total, stride)]
        got = lax.ppermute(message, "leaf", pairs)
        if bit == 0:
            return got, upper, halves[1]
        mine, next_mine = pack_width(bit, rank), pack_width(bit - 1, rank)
        held = size + mine if size else 2 * rank
        upper, message = kernel_call(
            functools.partial(spread_body, size, mine, next_mine, bit),
            [
                jax.ShapeDtypeStruct((rank, held), wide),
                jax.ShapeDtypeStruct((rank, max(held, next_mine)), wide),
            ],
            10**6,
            (spot, got, upper, *halves),
            scalars=1,
        )
        size = held


def solve(
    rhs_cols,
    leaf_inv,
    leaf_basis,
    leaf_back,
    leaf_coarse,
    mid_inv,
    mid_basis,
    mid_back,
    mid_coarse,
    top_inv,
    top_basis,
    top_back,
    top_coarse,
):
    leaf_count, height, _ = leaf_inv.shape
    rank, columns = leaf_basis.shape[2], rhs_cols.shape[1]
    position = lax.axis_index("leaf")
    leaf_total = lax.axis_size("leaf")
    depth = leaf_total.bit_length() - 1
    ring = lax.axis_size("rhs")
    ahead = [(i, (i + 1) % ring) for i in range(ring)]
    behind = [(i, (i - 1) % ring) for i in range(ring)]
    row = jnp.stack([lax.axis_index("rhs"), position]).astype(jnp.int32)

    own, whole = [], leaf_inv
    for start, count in PIECES:
        own.append(whole[start : start + count])
        if start == 0:
            whole, own[0], row = lax.optimization_barrier((whole, own[0], row))
    left = [lax.ppermute(a, "rhs", ahead) for a in own]
    right = [lax.ppermute(a, "rhs", behind) for a in own]
    pairs = ((left[0], right[1]), (left[2], right[3]))
    far = [
        (lax.ppermute(one, "rhs", ahead), lax.ppermute(two, "rhs", behind))
        for one, two in pairs
    ]

    got, upper, own_half = top_factors(
        top_inv[0], top_basis[0], top_back[0], top_coarse[0], row, depth
    )
    square = (rank, rank)
    up_first, down_first, up_x, down_x, down_y = kernel_call(
        top_body,
        [jax.ShapeDtypeStruct((rank, n * rank), wide) for n in (2, 2, 4, 4, 4)],
        10**8,
        (row, got, upper, own_half),
        scalars=1,
        scratch_shapes=[pltpu.VMEM((rank, upper.shape[1] + pack_width(0, rank)), wide)],
    )
    ups, paths = kernel_call(
        prepare_body,
        [
            jax.ShapeDtypeStruct((len(LATE), rank, 2 * rank), wide),
            jax.ShapeDtypeStruct((leaf_count, *square), wide),
        ],
        8 * 10**8,
        (mid_inv, mid_basis, mid_back, mid_coarse),
        room=12,
    )

    nears, parts = [], []
    for k in range(len(PIECES)):
        near, part = near_call(k, row, leaf_inv, left[k], right[k], rhs_cols, leaf_basis)
        nears.append(near)
        parts.append(part)
    shared = (rhs_cols, leaf_basis, leaf_coarse)
    first = kernel_call(
        functools.partial(far_leaves, 0),
        far_shapes(GROUPS[0][1], height, rank, columns),
        3 * 10**8,
        (row, *far[0], *shared, *parts[:2]),
        scalars=1,
    )
    early, early_base = kernel_call(
        merge_body,
        [
            jax.ShapeDtypeStruct((len(MERGED), rank, columns), wide),
            jax.ShapeDtypeStruct((len(MERGED), 2 * rank, columns), wide),
        ],
        len(MERGED) * 10**8,
        (first[2], mid_inv, mid_basis, mid_back, mid_coarse),
        room=12,
    )
    final = lax.optimization_barrier(
        (far[1], parts[2:], ups, early, up_first, down_first, up_x, down_x, down_y, paths)
    )
    (
        last_far, last_parts, ups, early, up_first, down_first, up_x, down_x, down_y, paths
    ) = final
    *last, late, current = kernel_call(
        last_body,
        far_shapes(GROUPS[1][1], height, rank, columns)
        + [
            jax.ShapeDtypeStruct((len(LATE) - 1, rank, columns), wide),
            jax.ShapeDtypeStruct((rank, columns), wide),
        ],
        4 * 10**8,
        (row, *last_far, *shared, *last_parts, ups, early),
        scalars=1,
    )
    late_base = kernel_call(
        late_body,
        jax.ShapeDtypeStruct((len(LATE), 2 * rank, columns), wide),
        6 * 10**8,
        (last[2], late, early, mid_inv, mid_basis, mid_back),
        room=12,
    )
    rest = kernel_call(
        known_body,
        jax.ShapeDtypeStruct((leaf_count, rank, columns), wide),
        4 * 10**8,
        (early_base, late_base, mid_back, first[1], last[1]),
        room=12,
    )

    def partners(value, masks):
        return [lax.ppermute(value, "leaf", [(i, i ^ m) for i in range(leaf_total)]) for m in masks]

    tall = jax.ShapeDtypeStruct((rank, columns), wide)
    first_pair = [current, *partners(current, (1,))]
    current = kernel_call(join_body, tall, 10**7, (up_first, *first_pair), room=6)
    along_x = [current, *partners(current, (2, 4, 6))]
    current = kernel_call(join_body, tall, 2 * 10**7, (up_x, *along_x), room=6)
    along_y = [current, *partners(current, (8, 16, 24))]
    below = kernel_call(
        below_body, tall, 10**7, (down_first, down_x, *first_pair, *along_x), room=6
    )
    top = kernel_call(end_body, tall, 10**7, (down_y, below, *along_y), room=6)
    return out_call(row, top, paths, rest, leaf_back, nears, (first[0], last[0]))


def solution(mesh):
    return jax.shard_map(
        solve,
        mesh=mesh,
        in_specs=(P("leaf", "rhs"), P("leaf", "rhs", None))
        + (P("leaf", None, None),) * 11,
        out_specs=P("leaf", "rhs"),
        check_vma=False,
    )
```

```python
import functools

import jax
import jax.numpy as jnp
from jax import lax
from jax.experimental import pallas as pl
from jax.experimental.pallas import tpu as pltpu
from jax.sharding import PartitionSpec as P


wide = jnp.float32
narrow = jnp.bfloat16

GROUPS = (tuple(range(8)), (8, 9, 12, 13), (10, 11, 14, 15))
PIECES = ((0, 4), (4, 4), (8, 4), (12, 4))
MERGED = (0, 1, 2, 3, 8, 9, 12)
LATE = (4, 5, 6, 7, 10, 11, 13, 14)
FRONT = (((0,), (0,)), ((), ()))


def narrow_dot(a, b):
    return jnp.dot(a.astype(narrow), b.astype(narrow), preferred_element_type=wide)


def parts_of(a):
    high = a.astype(narrow)
    return high, (a - high.astype(wide)).astype(narrow)


def split_dot(a, b, dims=(((1,), (0,)), ((), ()))):
    rows_at = 1 - dims[0][0][0]
    left = jnp.concatenate(parts_of(a), axis=rows_at)
    right = jnp.concatenate(parts_of(b), axis=1)
    full = lax.dot_general(left, right, dims, preferred_element_type=wide)
    m, n = a.shape[rows_at], b.shape[1]
    return (full[m:, n:] + full[m:, :n] + full[:m, n:]) + full[:m, :n]


def kernel_call(body, out_shape, flops, operands, scalars=0, room=10, **more):
    if scalars:
        more["in_specs"] = [pl.BlockSpec(memory_space=pltpu.SMEM)] * scalars + [
            pl.BlockSpec(a.shape, lambda a=a: (0,) * a.ndim) for a in operands[scalars:]
        ]
    size = sum(a.size * a.dtype.itemsize for a in operands)
    return pl.pallas_call(
        body,
        out_shape=out_shape,
        cost_estimate=pl.CostEstimate(flops=flops, bytes_accessed=size, transcendentals=0),
        compiler_params=pltpu.CompilerParams(vmem_limit_bytes=room * 1024 * 1024),
        **more,
    )(*operands)


def turned(row_ref, part, height):
    return pl.multiple_of(lax.rem(row_ref[0] + part, 4) * height, height)


def near_body(row_ref, own, left, right, rhs, basis, vals, proj):
    count, height, width = own.shape
    for k in range(count):
        rows = jnp.concatenate([own[k], left[k], right[k]], axis=0)
        got = narrow_dot(rows, rhs[k * width : (k + 1) * width, :])
        vals[k] = got.astype(narrow)
    at = [turned(row_ref, part, height) for part in (0, 3, 1)]
    for k in range(count):
        matching = jnp.concatenate([basis[k, pl.ds(a, height), :] for a in at], axis=0)
        proj[k] = lax.dot_general(matching, vals[k], FRONT, preferred_element_type=wide)


def near_call(piece, row, own, left, right, rhs, basis):
    start, count = PIECES[piece]
    height, width = left.shape[1:]
    rank, columns = basis.shape[2], rhs.shape[1]
    some = 4
    base = start // some

    def at(shape, shift):
        return pl.BlockSpec(shape, lambda i, row: (shift + i,) + (0,) * (len(shape) - 1))

    return pl.pallas_call(
        near_body,
        grid_spec=pltpu.PrefetchScalarGridSpec(
            num_scalar_prefetch=1,
            grid=(count // some,),
            in_specs=[
                at((some, height, width), base),
                at((some, height, width), 0),
                at((some, height, width), 0),
                at((some * width, columns), base),
                at((some, width, rank), base),
            ],
            out_specs=[
                at((some, 3 * height, columns), 0),
                at((some, rank, columns), 0),
            ],
        ),
        out_shape=[
            jax.ShapeDtypeStruct((count, 3 * height, columns), narrow),
            jax.ShapeDtypeStruct((count, rank, columns), wide),
        ],
        cost_estimate=pl.CostEstimate(
            flops=count * 2 * 3 * height * width * columns * 4,
            bytes_accessed=count * width * width * 2,
            transcendentals=0,
        ),
        compiler_params=pltpu.CompilerParams(vmem_limit_bytes=8 * 1024 * 1024),
    )(row, own, left, right, rhs, basis)


def far_leaves(
    group, row_ref, far_a, far_b, rhs, basis, coarse, part_a, part_b, vals, proj, lead
):
    leaves = GROUPS[group]
    height, width = far_a.shape[1], far_a.shape[2]
    half = len(leaves) // 2
    at = turned(row_ref, 2, height)
    for k, leaf in enumerate(leaves):
        rows = far_a[k] if k < half else far_b[k - half]
        got = narrow_dot(rows, rhs[leaf * width : (leaf + 1) * width, :])
        vals[k] = got.astype(narrow)
    for k, leaf in enumerate(leaves):
        before = (part_a if k < half else part_b)[leaf % 4]
        proj[k] = before + lax.dot_general(
            basis[leaf, pl.ds(at, height), :], vals[k], FRONT, preferred_element_type=wide
        )
    for k, leaf in enumerate(leaves):
        lead[k] = split_dot(coarse[leaf], proj[k])


def last_body(
    row_ref, far_a, far_b, rhs, basis, coarse, part_a, part_b, lead1, ups, early,
    vals, proj, lead, late, up,
):
    far_leaves(
        2, row_ref, far_a, far_b, rhs, basis, coarse, part_a, part_b, vals, proj, lead
    )
    value = {
        leaf: (ref, k) for g, ref in ((1, lead1), (2, lead)) for k, leaf in enumerate(GROUPS[g])
    }
    for k, node in enumerate(MERGED):
        value[16 + node] = (early, k)
    for k, node in enumerate(LATE):
        pair = [value[c][0][value[c][1]] for c in (2 * node, 2 * node + 1)]
        got = split_dot(ups[k], jnp.concatenate(pair, axis=0))
        if k == len(LATE) - 1:
            up[...] = got
        else:
            late[k] = got
        value[16 + node] = (late, k)


def far_shapes(count, height, rank, columns):
    return [
        jax.ShapeDtypeStruct((count, height, columns), narrow),
        jax.ShapeDtypeStruct((count, rank, columns), wide),
        jax.ShapeDtypeStruct((count, rank, columns), wide),
    ]


def by_level(nodes):
    for first, last in ((0, 8), (8, 12), (12, 14), (14, 15)):
        level = [(k, node) for k, node in enumerate(nodes) if first <= node < last]
        if level:
            yield level


def merge_body(lead, inv, basis, back, coarse, early, base):
    value = {k: (lead, k) for k in range(lead.shape[0])}
    for level in by_level(MERGED):
        solved, reduced = {}, {}
        for k, node in level:
            pair = [value[c][0][value[c][1]] for c in (2 * node, 2 * node + 1)]
            solved[k] = split_dot(inv[node], jnp.concatenate(pair, axis=0))
        for k, node in level:
            reduced[k] = split_dot(basis[node], solved[k], FRONT)
        for k, node in level:
            early[k] = split_dot(coarse[node], reduced[k])
            base[k] = solved[k] - split_dot(back[node], reduced[k])
            value[16 + node] = (early, k)


def prepare_body(inv, basis, back, coarse, ups, paths):
    for k, node in enumerate(LATE):
        ups[k] = split_dot(coarse[node], split_dot(basis[node], inv[node], FRONT))
    value = {30: None}
    rank = paths.shape[1]
    for node in reversed(range(15)):
        above = value[16 + node]
        below = back[node] if above is None else split_dot(back[node], above)
        for k in range(2):
            value[2 * node + k] = below[k * rank : (k + 1) * rank]
            if node < 8:
                paths[2 * node + k] = value[2 * node + k]


def late_body(lead1, lead2, late, early, inv, basis, back, base):
    value = {
        leaf: (ref, k) for g, ref in ((1, lead1), (2, lead2)) for k, leaf in enumerate(GROUPS[g])
    }
    for k, node in enumerate(MERGED):
        value[16 + node] = (early, k)
    for k, node in enumerate(LATE[:-1]):
        value[16 + node] = (late, k)
    reduced = {}
    for k, node in enumerate(LATE):
        pair = [value[c][0][value[c][1]] for c in (2 * node, 2 * node + 1)]
        base[k] = split_dot(inv[node], jnp.concatenate(pair, axis=0))
    for k, node in enumerate(LATE):
        reduced[k] = split_dot(basis[node], base[k], FRONT)
    for k, node in enumerate(LATE):
        base[k] -= split_dot(back[node], reduced[k])


def known_body(base0, base1, back, proj0, proj1, proj2, rest):
    rank = proj0.shape[1]
    known = {}
    for base, nodes in ((base0, MERGED), (base1, LATE)):
        for k, node in enumerate(nodes):
            known[node] = (base, k)
    projs = {
        leaf: (ref, k)
        for ref, leaves in zip((proj0, proj1, proj2), GROUPS)
        for k, leaf in enumerate(leaves)
    }
    part = {30: None}
    for node in reversed(range(15)):
        ref, at = known[node]
        halves = ref[at]
        if part[16 + node] is not None:
            halves = halves + split_dot(back[node], part[16 + node])
        for k in range(2):
            below = halves[k * rank : (k + 1) * rank]
            part[2 * node + k] = below
            if node < 8:
                ref, at = projs[2 * node + k]
                rest[2 * node + k] = ref[at] - below


def spread_body(size, mine, next_mine, bit, spot, got, upper, low_half, high_half, wider, message):
    high, next_high = (lax.rem(spot[1] >> b, 2) == 1 for b in (bit, bit - 1))
    if size:
        wider[:, :size] = jnp.where(high, got[:, :size], upper[...])
        wider[:, size:] = jnp.where(high, high_half[:, :mine], got[:, :mine])
    else:
        wider[...] = jnp.where(high, upper[...], got[...])
    held = wider.shape[1]
    both = min(next_mine, held)
    message[:, :both] = jnp.where(next_high, low_half[:, :both], wider[:, :both])
    if next_mine > held:
        message[:, held:] = low_half[:, held:next_mine]
    if held > next_mine:
        message[:, next_mine:] = wider[:, next_mine:]


def top_body(spot, got, upper, high_half, up_first, down_first, up_x, down_x, down_y, packs):
    rank = packs.shape[0]
    size = upper.shape[1]
    mine = pack_width(0, rank)
    high = lax.rem(spot[1], 2) == 1
    packs[:, :size] = jnp.where(high, got[:, :size], upper[...])
    packs[:, size:] = jnp.where(high, high_half[:, :mine], got[:, :mine])

    def sided(level, matrix):
        is_left = lax.rem(spot[1] >> level, 2) == 0
        one, two = matrix[:, :rank], matrix[:, rank:]
        return jnp.concatenate(
            [jnp.where(is_left, one, two), jnp.where(is_left, two, one)], axis=1
        )

    ups, downs, sibling, path = {}, {}, {}, None
    end = packs.shape[1]
    for level in range(4):
        first = end - pack_width(level, rank)
        end = first
        ups[level] = sided(level, packs[:, first : first + 2 * rank])
        down = packs[:, first + 2 * rank : first + 4 * rank]
        downs[level] = sided(level, down if path is None else split_dot(path, down))
        step = packs[:, first + 4 * rank : first + 5 * rank]
        path = step if path is None else split_dot(path, step)
        if level % 2:
            sibling[level] = sided(level, packs[:, first + 5 * rank : first + 7 * rank])
    downs[4] = sided(4, split_dot(path, packs[:, : 2 * rank]))

    def joined(above, low):
        near = split_dot(above[:, :rank], ups[low])
        return near, split_dot(above[:, rank:], sibling[low])

    up_first[...] = ups[0]
    down_first[...] = downs[0]
    up_x[:, : 2 * rank], up_x[:, 2 * rank :] = joined(ups[2], 1)
    for out, low in ((down_x, 1), (down_y, 3)):
        near, away = joined(downs[low + 1], low)
        out[:, : 2 * rank] = downs[low] + near
        out[:, 2 * rank :] = away


def join_body(matrix, *refs):
    refs[-1][...] = split_dot(
        matrix[...], jnp.concatenate([r[...] for r in refs[:-1]], axis=0)
    )


def below_body(first, second, *refs):
    out = refs[-1]
    out[...] = split_dot(
        first[...], jnp.concatenate([r[...] for r in refs[:2]], axis=0)
    ) + split_dot(second[...], jnp.concatenate([r[...] for r in refs[2:-1]], axis=0))


def pack_width(bit, rank):
    return (7 if bit % 2 else 5) * rank


def out_body(
    row_ref, down_y, below, here, one, two, three, paths, rest, back,
    near0, near1, near2, near3, far0, far1, far2, out, blocks, sent,
):
    leaves, width = back.shape[0], back.shape[1]
    height = far0.shape[1]
    along = jnp.concatenate([here[...], one[...], two[...], three[...]], axis=0)
    top = below[...] + split_dot(down_y[...], along)
    at = [turned(row_ref, part, height) for part in (0, 3, 1, 2)]
    spans = zip(PIECES, (near0, near1, near2, near3))
    nears = [(ref, k) for (_, count), ref in spans for k in range(count)]
    fars = {
        leaf: (ref, k)
        for ref, group in zip((far0, far1, far2), GROUPS)
        for k, leaf in enumerate(group)
    }
    copies = [
        pltpu.make_async_copy(
            blocks.at[leaf], out.at[pl.ds(leaf * width, width), :], sent.at[leaf]
        )
        for leaf in range(leaves)
    ]
    rank, some = top.shape[0], 4
    for leaf in range(leaves):
        k = leaf % some
        if k == 0:
            these = paths[leaf : leaf + some].reshape(some * rank, rank)
            down = split_dot(these, top)
        difference = (rest[leaf] - down[k * rank : (k + 1) * rank]).astype(narrow)
        matching = jnp.concatenate([back[leaf, pl.ds(a, height), :] for a in at], axis=0)
        change = narrow_dot(matching, difference)
        near, far = nears[leaf], fars[leaf]
        for j, a in enumerate(at):
            if j == 3:
                block = far[0][far[1]]
            else:
                block = near[0][near[1], j * height : (j + 1) * height, :]
            blocks[leaf, pl.ds(a, height), :] = (
                block.astype(wide) - change[j * height : (j + 1) * height]
            )
        if leaf:
            copies[leaf - 1].start()
    copies[-1].start()
    for copy in copies:
        copy.wait()


def exact(eq, a, b):
    return jnp.einsum(eq, a, b, precision=lax.Precision.HIGHEST)


def top_factors(inv, basis, back, coarse, spot, depth):
    total = lax.axis_size("leaf")
    rank = basis.shape[1]
    reduce_mat = exact("ik,ij->kj", basis, inv)
    up_mat = exact("kl,lj->kj", coarse, reduce_mat)
    down_mat = inv - exact("ik,kj->ij", back, reduce_mat)
    swaps = [
        (i, i ^ (2 * stride)) for stride in (2, 8) for i in range(stride, total, 2 * stride)
    ]
    swapped = lax.ppermute(up_mat, "leaf", swaps)
    halves = [
        jnp.concatenate([up_mat, down_mat[s : s + rank], back[s : s + rank], swapped], axis=1)
        for s in (0, rank)
    ]
    upper, message, size = inv[rank:], inv[:rank], 0
    for bit in reversed(range(depth)):
        stride = 1 << bit
        if size == 0:
            pairs = [(stride, 0)]
        else:
            pairs = [(i, i ^ stride) for i in range(0, total, stride)]
        got = lax.ppermute(message, "leaf", pairs)
        if bit == 0:
            return got, upper, halves[1]
        mine, next_mine = pack_width(bit, rank), pack_width(bit - 1, rank)
        held = size + mine if size else 2 * rank
        upper, message = kernel_call(
            functools.partial(spread_body, size, mine, next_mine, bit),
            [
                jax.ShapeDtypeStruct((rank, held), wide),
                jax.ShapeDtypeStruct((rank, max(held, next_mine)), wide),
            ],
            10**6,
            (spot, got, upper, *halves),
            scalars=1,
        )
        size = held


def solve(
    rhs_cols,
    leaf_inv,
    leaf_basis,
    leaf_back,
    leaf_coarse,
    mid_inv,
    mid_basis,
    mid_back,
    mid_coarse,
    top_inv,
    top_basis,
    top_back,
    top_coarse,
):
    leaf_count, height, width = leaf_inv.shape
    rank, columns = leaf_basis.shape[2], rhs_cols.shape[1]
    position = lax.axis_index("leaf")
    leaf_total = lax.axis_size("leaf")
    depth = leaf_total.bit_length() - 1
    ring = lax.axis_size("rhs")
    ahead = [(i, (i + 1) % ring) for i in range(ring)]
    behind = [(i, (i - 1) % ring) for i in range(ring)]
    row = jnp.stack([lax.axis_index("rhs"), position]).astype(jnp.int32)

    own, whole = [], leaf_inv
    for start, count in PIECES:
        own.append(whole[start : start + count])
        if start == 0:
            whole, own[0], row = lax.optimization_barrier((whole, own[0], row))
    left = [lax.ppermute(a, "rhs", ahead) for a in own]
    right = [lax.ppermute(a, "rhs", behind) for a in own]
    pairs = ((left[0], right[1]), (left[2][:2], right[3][:2]), (left[2][2:], right[3][2:]))
    far = [
        (lax.ppermute(one, "rhs", ahead), lax.ppermute(two, "rhs", behind))
        for one, two in pairs
    ]

    got, upper, own_half = top_factors(
        top_inv[0], top_basis[0], top_back[0], top_coarse[0], row, depth
    )
    square = (rank, rank)
    up_first, down_first, up_x, down_x, down_y = kernel_call(
        top_body,
        [jax.ShapeDtypeStruct((rank, n * rank), wide) for n in (2, 2, 4, 4, 4)],
        10**8,
        (row, got, upper, own_half),
        scalars=1,
        scratch_shapes=[pltpu.VMEM((rank, upper.shape[1] + pack_width(0, rank)), wide)],
    )
    ups, paths = kernel_call(
        prepare_body,
        [
            jax.ShapeDtypeStruct((len(LATE), rank, 2 * rank), wide),
            jax.ShapeDtypeStruct((leaf_count, *square), wide),
        ],
        8 * 10**8,
        (mid_inv, mid_basis, mid_back, mid_coarse),
        room=12,
    )

    nears, parts = [], []
    for k in range(len(PIECES)):
        near, part = near_call(k, row, leaf_inv, left[k], right[k], rhs_cols, leaf_basis)
        nears.append(near)
        parts.append(part)
    shared = (rhs_cols, leaf_basis, leaf_coarse)
    first = kernel_call(
        functools.partial(far_leaves, 0),
        far_shapes(len(GROUPS[0]), height, rank, columns),
        3 * 10**8,
        (row, *far[0], *shared, *parts[:2]),
        scalars=1,
    )
    second = kernel_call(
        functools.partial(far_leaves, 1),
        far_shapes(len(GROUPS[1]), height, rank, columns),
        15 * 10**7,
        (row, *far[1], *shared, *parts[2:]),
        scalars=1,
    )
    early, early_base = kernel_call(
        merge_body,
        [
            jax.ShapeDtypeStruct((len(MERGED), rank, columns), wide),
            jax.ShapeDtypeStruct((len(MERGED), 2 * rank, columns), wide),
        ],
        len(MERGED) * 10**8,
        (first[2], mid_inv, mid_basis, mid_back, mid_coarse),
        room=12,
    )
    final = lax.optimization_barrier(
        (far[2], parts[2:], second[2], ups, early, up_first, down_first, up_x, down_x, down_y, paths)
    )
    (
        last_far, last_parts, second_lead, ups, early, up_first, down_first, up_x, down_x, down_y, paths
    ) = final
    *last, late, current = kernel_call(
        last_body,
        far_shapes(len(GROUPS[2]), height, rank, columns)
        + [
            jax.ShapeDtypeStruct((len(LATE) - 1, rank, columns), wide),
            jax.ShapeDtypeStruct((rank, columns), wide),
        ],
        4 * 10**8,
        (row, *last_far, *shared, *last_parts, second_lead, ups, early),
        scalars=1,
    )
    late_base = kernel_call(
        late_body,
        jax.ShapeDtypeStruct((len(LATE), 2 * rank, columns), wide),
        6 * 10**8,
        (second_lead, last[2], late, early, mid_inv, mid_basis, mid_back),
        room=12,
    )
    rest = kernel_call(
        known_body,
        jax.ShapeDtypeStruct((leaf_count, rank, columns), wide),
        4 * 10**8,
        (early_base, late_base, mid_back, first[1], second[1], last[1]),
        room=12,
    )

    def partners(value, masks):
        return [lax.ppermute(value, "leaf", [(i, i ^ m) for i in range(leaf_total)]) for m in masks]

    tall = jax.ShapeDtypeStruct((rank, columns), wide)
    first_pair = [current, *partners(current, (1,))]
    current = kernel_call(join_body, tall, 10**7, (up_first, *first_pair), room=6)
    along_x = [current, *partners(current, (2, 4, 6))]
    current = kernel_call(join_body, tall, 2 * 10**7, (up_x, *along_x), room=6)
    along_y = [current, *partners(current, (8, 16, 24))]
    below = kernel_call(
        below_body, tall, 10**7, (down_first, down_x, *first_pair, *along_x), room=6
    )
    return kernel_call(
        out_body,
        jax.ShapeDtypeStruct((leaf_count * width, columns), wide),
        10**9,
        (
            row,
            down_y,
            below,
            *along_y,
            paths,
            rest,
            leaf_back,
            *nears,
            first[0],
            second[0],
            last[0],
        ),
        scalars=1,
        room=12,
        out_specs=pl.BlockSpec(memory_space=pl.ANY),
        scratch_shapes=[
            pltpu.VMEM((leaf_count, width, columns), wide),
            pltpu.SemaphoreType.DMA((leaf_count,)),
        ],
    )


def solution(mesh):
    return jax.shard_map(
        solve,
        mesh=mesh,
        in_specs=(P("leaf", "rhs"), P("leaf", "rhs", None))
        + (P("leaf", None, None),) * 11,
        out_specs=P("leaf", "rhs"),
        check_vma=False,
    )
```

```python
import functools

import jax
import jax.numpy as jnp
from jax import lax
from jax.experimental import pallas as pl
from jax.experimental.pallas import tpu as pltpu
from jax.sharding import PartitionSpec as P


wide = jnp.float32
narrow = jnp.bfloat16

GROUPS = ((0, 8), (8, 8))
PIECES = ((0, 4), (4, 4), (8, 4), (12, 4))
MERGED = (0, 1, 2, 3, 8, 9, 12)
LATE = (4, 5, 6, 7, 10, 11, 13, 14)
FRONT = (((0,), (0,)), ((), ()))


def narrow_dot(a, b):
    return jnp.dot(a.astype(narrow), b.astype(narrow), preferred_element_type=wide)


def parts_of(a):
    high = a.astype(narrow)
    return high, (a - high.astype(wide)).astype(narrow)


def split_dot(a, b, dims=(((1,), (0,)), ((), ()))):
    rows_at = 1 - dims[0][0][0]
    left = jnp.concatenate(parts_of(a), axis=rows_at)
    right = jnp.concatenate(parts_of(b), axis=1)
    full = lax.dot_general(left, right, dims, preferred_element_type=wide)
    m, n = a.shape[rows_at], b.shape[1]
    return (full[m:, n:] + full[m:, :n] + full[:m, n:]) + full[:m, :n]


def kernel_call(body, out_shape, flops, operands, scalars=0, room=10, **more):
    if scalars:
        more["in_specs"] = [pl.BlockSpec(memory_space=pltpu.SMEM)] * scalars + [
            pl.BlockSpec(a.shape, lambda a=a: (0,) * a.ndim) for a in operands[scalars:]
        ]
    size = sum(a.size * a.dtype.itemsize for a in operands)
    return pl.pallas_call(
        body,
        out_shape=out_shape,
        cost_estimate=pl.CostEstimate(flops=flops, bytes_accessed=size, transcendentals=0),
        compiler_params=pltpu.CompilerParams(vmem_limit_bytes=room * 1024 * 1024),
        **more,
    )(*operands)


def turned(row_ref, part, height):
    return pl.multiple_of(lax.rem(row_ref[0] + part, 4) * height, height)


def near_body(row_ref, own, left, right, rhs, basis, vals, proj):
    count, height, width = own.shape
    for k in range(count):
        rows = jnp.concatenate([own[k], left[k], right[k]], axis=0)
        got = narrow_dot(rows, rhs[k * width : (k + 1) * width, :])
        vals[k] = got.astype(narrow)
    at = [turned(row_ref, part, height) for part in (0, 3, 1)]
    for k in range(count):
        matching = jnp.concatenate([basis[k, pl.ds(a, height), :] for a in at], axis=0)
        proj[k] = lax.dot_general(matching, vals[k], FRONT, preferred_element_type=wide)


def near_call(piece, row, own, left, right, rhs, basis):
    start, count = PIECES[piece]
    height, width = left.shape[1:]
    rank, columns = basis.shape[2], rhs.shape[1]
    some = 4
    base = start // some

    def at(shape, shift):
        return pl.BlockSpec(shape, lambda i, row: (shift + i,) + (0,) * (len(shape) - 1))

    return pl.pallas_call(
        near_body,
        grid_spec=pltpu.PrefetchScalarGridSpec(
            num_scalar_prefetch=1,
            grid=(count // some,),
            in_specs=[
                at((some, height, width), base),
                at((some, height, width), 0),
                at((some, height, width), 0),
                at((some * width, columns), base),
                at((some, width, rank), base),
            ],
            out_specs=[
                at((some, 3 * height, columns), 0),
                at((some, rank, columns), 0),
            ],
        ),
        out_shape=[
            jax.ShapeDtypeStruct((count, 3 * height, columns), narrow),
            jax.ShapeDtypeStruct((count, rank, columns), wide),
        ],
        cost_estimate=pl.CostEstimate(
            flops=count * 2 * 3 * height * width * columns * 4,
            bytes_accessed=count * width * width * 2,
            transcendentals=0,
        ),
        compiler_params=pltpu.CompilerParams(vmem_limit_bytes=8 * 1024 * 1024),
    )(row, own, left, right, rhs, basis)


def far_leaves(
    group, row_ref, far_a, far_b, rhs, basis, coarse, part_a, part_b, vals, proj, lead
):
    start, count = GROUPS[group]
    height, width = far_a.shape[1], far_a.shape[2]
    half = count // 2
    at = turned(row_ref, 2, height)
    for k in range(count):
        leaf = start + k
        rows = far_a[k] if k < half else far_b[k - half]
        got = narrow_dot(rows, rhs[leaf * width : (leaf + 1) * width, :])
        vals[k] = got.astype(narrow)
    for k in range(count):
        before = part_a[k] if k < half else part_b[k - half]
        proj[k] = before + lax.dot_general(
            basis[start + k, pl.ds(at, height), :], vals[k], FRONT, preferred_element_type=wide
        )
    for k in range(count):
        lead[k] = split_dot(coarse[start + k], proj[k])


def last_body(
    row_ref, far_a, far_b, rhs, basis, coarse, part_a, part_b, ups, early,
    vals, proj, lead, late, up,
):
    far_leaves(
        1, row_ref, far_a, far_b, rhs, basis, coarse, part_a, part_b, vals, proj, lead
    )
    value = {8 + k: (lead, k) for k in range(8)}
    for k, node in enumerate(MERGED):
        value[16 + node] = (early, k)
    for k, node in enumerate(LATE):
        pair = [value[c][0][value[c][1]] for c in (2 * node, 2 * node + 1)]
        got = split_dot(ups[k], jnp.concatenate(pair, axis=0))
        if k == len(LATE) - 1:
            up[...] = got
        else:
            late[k] = got
        value[16 + node] = (late, k)


def far_shapes(count, height, rank, columns):
    return [
        jax.ShapeDtypeStruct((count, height, columns), narrow),
        jax.ShapeDtypeStruct((count, rank, columns), wide),
        jax.ShapeDtypeStruct((count, rank, columns), wide),
    ]


def by_level(nodes):
    for first, last in ((0, 8), (8, 12), (12, 14), (14, 15)):
        level = [(k, node) for k, node in enumerate(nodes) if first <= node < last]
        if level:
            yield level


def merge_body(lead, inv, basis, back, coarse, early, base):
    value = {k: (lead, k) for k in range(lead.shape[0])}
    for level in by_level(MERGED):
        solved, reduced = {}, {}
        for k, node in level:
            pair = [value[c][0][value[c][1]] for c in (2 * node, 2 * node + 1)]
            solved[k] = split_dot(inv[node], jnp.concatenate(pair, axis=0))
        for k, node in level:
            reduced[k] = split_dot(basis[node], solved[k], FRONT)
        for k, node in level:
            early[k] = split_dot(coarse[node], reduced[k])
            base[k] = solved[k] - split_dot(back[node], reduced[k])
            value[16 + node] = (early, k)


def prepare_body(inv, basis, back, coarse, ups, paths):
    for k, node in enumerate(LATE):
        ups[k] = split_dot(coarse[node], split_dot(basis[node], inv[node], FRONT))
    value = {30: None}
    rank = paths.shape[1]
    for node in reversed(range(15)):
        above = value[16 + node]
        below = back[node] if above is None else split_dot(back[node], above)
        for k in range(2):
            value[2 * node + k] = below[k * rank : (k + 1) * rank]
            if node < 8:
                paths[2 * node + k] = value[2 * node + k]


def late_body(lead, late, early, inv, basis, back, base):
    value = {8 + k: (lead, k) for k in range(8)}
    for k, node in enumerate(MERGED):
        value[16 + node] = (early, k)
    for k, node in enumerate(LATE[:-1]):
        value[16 + node] = (late, k)
    reduced = {}
    for k, node in enumerate(LATE):
        pair = [value[c][0][value[c][1]] for c in (2 * node, 2 * node + 1)]
        base[k] = split_dot(inv[node], jnp.concatenate(pair, axis=0))
    for k, node in enumerate(LATE):
        reduced[k] = split_dot(basis[node], base[k], FRONT)
    for k, node in enumerate(LATE):
        base[k] -= split_dot(back[node], reduced[k])


def known_body(base0, base1, back, proj0, proj1, rest):
    rank = proj0.shape[1]
    known = {}
    for base, nodes in ((base0, MERGED), (base1, LATE)):
        for k, node in enumerate(nodes):
            known[node] = (base, k)
    projs = [(proj, k) for proj in (proj0, proj1) for k in range(proj.shape[0])]
    part = {30: None}
    for node in reversed(range(15)):
        ref, at = known[node]
        halves = ref[at]
        if part[16 + node] is not None:
            halves = halves + split_dot(back[node], part[16 + node])
        for k in range(2):
            below = halves[k * rank : (k + 1) * rank]
            part[2 * node + k] = below
            if node < 8:
                ref, at = projs[2 * node + k]
                rest[2 * node + k] = ref[at] - below


def spread_body(size, mine, next_mine, bit, spot, got, upper, low_half, high_half, wider, message):
    high, next_high = (lax.rem(spot[1] >> b, 2) == 1 for b in (bit, bit - 1))
    if size:
        wider[:, :size] = jnp.where(high, got[:, :size], upper[...])
        wider[:, size:] = jnp.where(high, high_half[:, :mine], got[:, :mine])
    else:
        wider[...] = jnp.where(high, upper[...], got[...])
    held = wider.shape[1]
    both = min(next_mine, held)
    message[:, :both] = jnp.where(next_high, low_half[:, :both], wider[:, :both])
    if next_mine > held:
        message[:, held:] = low_half[:, held:next_mine]
    if held > next_mine:
        message[:, next_mine:] = wider[:, next_mine:]


def top_body(spot, got, upper, high_half, up_first, down_first, up_x, down_x, down_y, packs):
    rank = packs.shape[0]
    size = upper.shape[1]
    mine = pack_width(0, rank)
    high = lax.rem(spot[1], 2) == 1
    packs[:, :size] = jnp.where(high, got[:, :size], upper[...])
    packs[:, size:] = jnp.where(high, high_half[:, :mine], got[:, :mine])

    def sided(level, matrix):
        is_left = lax.rem(spot[1] >> level, 2) == 0
        one, two = matrix[:, :rank], matrix[:, rank:]
        return jnp.concatenate(
            [jnp.where(is_left, one, two), jnp.where(is_left, two, one)], axis=1
        )

    ups, downs, sibling, path = {}, {}, {}, None
    end = packs.shape[1]
    for level in range(4):
        first = end - pack_width(level, rank)
        end = first
        ups[level] = sided(level, packs[:, first : first + 2 * rank])
        down = packs[:, first + 2 * rank : first + 4 * rank]
        downs[level] = sided(level, down if path is None else split_dot(path, down))
        step = packs[:, first + 4 * rank : first + 5 * rank]
        path = step if path is None else split_dot(path, step)
        if level % 2:
            sibling[level] = sided(level, packs[:, first + 5 * rank : first + 7 * rank])
    downs[4] = sided(4, split_dot(path, packs[:, : 2 * rank]))

    def joined(above, low):
        near = split_dot(above[:, :rank], ups[low])
        return near, split_dot(above[:, rank:], sibling[low])

    up_first[...] = ups[0]
    down_first[...] = downs[0]
    up_x[:, : 2 * rank], up_x[:, 2 * rank :] = joined(ups[2], 1)
    for out, low in ((down_x, 1), (down_y, 3)):
        near, away = joined(downs[low + 1], low)
        out[:, : 2 * rank] = downs[low] + near
        out[:, 2 * rank :] = away


def join_body(matrix, *refs):
    refs[-1][...] = split_dot(
        matrix[...], jnp.concatenate([r[...] for r in refs[:-1]], axis=0)
    )


def below_body(first, second, *refs):
    out = refs[-1]
    out[...] = split_dot(
        first[...], jnp.concatenate([r[...] for r in refs[:2]], axis=0)
    ) + split_dot(second[...], jnp.concatenate([r[...] for r in refs[2:-1]], axis=0))


def pack_width(bit, rank):
    return (7 if bit % 2 else 5) * rank


def out_body(
    row_ref, down_y, below, here, one, two, three, paths, rest, back,
    near0, near1, near2, near3, far0, far1, out, blocks, sent,
):
    leaves, width = back.shape[0], back.shape[1]
    height = far0.shape[1]
    along = jnp.concatenate([here[...], one[...], two[...], three[...]], axis=0)
    top = below[...] + split_dot(down_y[...], along)
    at = [turned(row_ref, part, height) for part in (0, 3, 1, 2)]
    spans = zip(PIECES, (near0, near1, near2, near3))
    nears = [(ref, k) for (_, count), ref in spans for k in range(count)]
    fars = [(ref, k) for (_, count), ref in zip(GROUPS, (far0, far1)) for k in range(count)]
    copies = [
        pltpu.make_async_copy(
            blocks.at[leaf], out.at[pl.ds(leaf * width, width), :], sent.at[leaf]
        )
        for leaf in range(leaves)
    ]
    for leaf in range(leaves):
        difference = (rest[leaf] - split_dot(paths[leaf], top)).astype(narrow)
        matching = jnp.concatenate([back[leaf, pl.ds(a, height), :] for a in at], axis=0)
        change = narrow_dot(matching, difference)
        near, far = nears[leaf], fars[leaf]
        for j, a in enumerate(at):
            if j == 3:
                block = far[0][far[1]]
            else:
                block = near[0][near[1], j * height : (j + 1) * height, :]
            blocks[leaf, pl.ds(a, height), :] = (
                block.astype(wide) - change[j * height : (j + 1) * height]
            )
        copies[leaf].start()
    for copy in copies:
        copy.wait()


def exact(eq, a, b):
    return jnp.einsum(eq, a, b, precision=lax.Precision.HIGHEST)


def top_factors(inv, basis, back, coarse, spot, depth):
    total = lax.axis_size("leaf")
    rank = basis.shape[1]
    reduce_mat = exact("ik,ij->kj", basis, inv)
    up_mat = exact("kl,lj->kj", coarse, reduce_mat)
    down_mat = inv - exact("ik,kj->ij", back, reduce_mat)
    swaps = [
        (i, i ^ (2 * stride)) for stride in (2, 8) for i in range(stride, total, 2 * stride)
    ]
    swapped = lax.ppermute(up_mat, "leaf", swaps)
    halves = [
        jnp.concatenate([up_mat, down_mat[s : s + rank], back[s : s + rank], swapped], axis=1)
        for s in (0, rank)
    ]
    upper, message, size = inv[rank:], inv[:rank], 0
    for bit in reversed(range(depth)):
        stride = 1 << bit
        if size == 0:
            pairs = [(stride, 0)]
        else:
            pairs = [(i, i ^ stride) for i in range(0, total, stride)]
        got = lax.ppermute(message, "leaf", pairs)
        if bit == 0:
            return got, upper, halves[1]
        mine, next_mine = pack_width(bit, rank), pack_width(bit - 1, rank)
        held = size + mine if size else 2 * rank
        upper, message = kernel_call(
            functools.partial(spread_body, size, mine, next_mine, bit),
            [
                jax.ShapeDtypeStruct((rank, held), wide),
                jax.ShapeDtypeStruct((rank, max(held, next_mine)), wide),
            ],
            10**6,
            (spot, got, upper, *halves),
            scalars=1,
        )
        size = held


def solve(
    rhs_cols,
    leaf_inv,
    leaf_basis,
    leaf_back,
    leaf_coarse,
    mid_inv,
    mid_basis,
    mid_back,
    mid_coarse,
    top_inv,
    top_basis,
    top_back,
    top_coarse,
):
    leaf_count, height, width = leaf_inv.shape
    rank, columns = leaf_basis.shape[2], rhs_cols.shape[1]
    position = lax.axis_index("leaf")
    leaf_total = lax.axis_size("leaf")
    depth = leaf_total.bit_length() - 1
    ring = lax.axis_size("rhs")
    ahead = [(i, (i + 1) % ring) for i in range(ring)]
    behind = [(i, (i - 1) % ring) for i in range(ring)]
    row = jnp.stack([lax.axis_index("rhs"), position]).astype(jnp.int32)

    own, whole = [], leaf_inv
    for start, count in PIECES:
        own.append(whole[start : start + count])
        if start == 0:
            whole, own[0], row = lax.optimization_barrier((whole, own[0], row))
    left = [lax.ppermute(a, "rhs", ahead) for a in own]
    right = [lax.ppermute(a, "rhs", behind) for a in own]
    pairs = ((left[0], right[1]), (left[2], right[3]))
    far = [
        (lax.ppermute(one, "rhs", ahead), lax.ppermute(two, "rhs", behind))
        for one, two in pairs
    ]

    got, upper, own_half = top_factors(
        top_inv[0], top_basis[0], top_back[0], top_coarse[0], row, depth
    )
    square = (rank, rank)
    up_first, down_first, up_x, down_x, down_y = kernel_call(
        top_body,
        [jax.ShapeDtypeStruct((rank, n * rank), wide) for n in (2, 2, 4, 4, 4)],
        10**8,
        (row, got, upper, own_half),
        scalars=1,
        scratch_shapes=[pltpu.VMEM((rank, upper.shape[1] + pack_width(0, rank)), wide)],
    )
    ups, paths = kernel_call(
        prepare_body,
        [
            jax.ShapeDtypeStruct((len(LATE), rank, 2 * rank), wide),
            jax.ShapeDtypeStruct((leaf_count, *square), wide),
        ],
        8 * 10**8,
        (mid_inv, mid_basis, mid_back, mid_coarse),
        room=12,
    )

    nears, parts = [], []
    for k in range(len(PIECES)):
        near, part = near_call(k, row, leaf_inv, left[k], right[k], rhs_cols, leaf_basis)
        nears.append(near)
        parts.append(part)
    shared = (rhs_cols, leaf_basis, leaf_coarse)
    first = kernel_call(
        functools.partial(far_leaves, 0),
        far_shapes(GROUPS[0][1], height, rank, columns),
        3 * 10**8,
        (row, *far[0], *shared, *parts[:2]),
        scalars=1,
    )
    early, early_base = kernel_call(
        merge_body,
        [
            jax.ShapeDtypeStruct((len(MERGED), rank, columns), wide),
            jax.ShapeDtypeStruct((len(MERGED), 2 * rank, columns), wide),
        ],
        len(MERGED) * 10**8,
        (first[2], mid_inv, mid_basis, mid_back, mid_coarse),
        room=12,
    )
    final = lax.optimization_barrier(
        (far[1], parts[2:], ups, early, up_first, down_first, up_x, down_x, down_y, paths)
    )
    (
        last_far, last_parts, ups, early, up_first, down_first, up_x, down_x, down_y, paths
    ) = final
    *last, late, current = kernel_call(
        last_body,
        far_shapes(GROUPS[1][1], height, rank, columns)
        + [
            jax.ShapeDtypeStruct((len(LATE) - 1, rank, columns), wide),
            jax.ShapeDtypeStruct((rank, columns), wide),
        ],
        4 * 10**8,
        (row, *last_far, *shared, *last_parts, ups, early),
        scalars=1,
    )
    late_base = kernel_call(
        late_body,
        jax.ShapeDtypeStruct((len(LATE), 2 * rank, columns), wide),
        6 * 10**8,
        (last[2], late, early, mid_inv, mid_basis, mid_back),
        room=12,
    )
    rest = kernel_call(
        known_body,
        jax.ShapeDtypeStruct((leaf_count, rank, columns), wide),
        4 * 10**8,
        (early_base, late_base, mid_back, first[1], last[1]),
        room=12,
    )

    def partners(value, masks):
        return [lax.ppermute(value, "leaf", [(i, i ^ m) for i in range(leaf_total)]) for m in masks]

    tall = jax.ShapeDtypeStruct((rank, columns), wide)
    first_pair = [current, *partners(current, (1,))]
    current = kernel_call(join_body, tall, 10**7, (up_first, *first_pair), room=6)
    along_x = [current, *partners(current, (2, 4, 6))]
    current = kernel_call(join_body, tall, 2 * 10**7, (up_x, *along_x), room=6)
    along_y = [current, *partners(current, (8, 16, 24))]
    below = kernel_call(
        below_body, tall, 10**7, (down_first, down_x, *first_pair, *along_x), room=6
    )
    return kernel_call(
        out_body,
        jax.ShapeDtypeStruct((leaf_count * width, columns), wide),
        10**9,
        (
            row,
            down_y,
            below,
            *along_y,
            paths,
            rest,
            leaf_back,
            *nears,
            first[0],
            last[0],
        ),
        scalars=1,
        room=12,
        out_specs=pl.BlockSpec(memory_space=pl.ANY),
        scratch_shapes=[
            pltpu.VMEM((leaf_count, width, columns), wide),
            pltpu.SemaphoreType.DMA((leaf_count,)),
        ],
    )


def solution(mesh):
    return jax.shard_map(
        solve,
        mesh=mesh,
        in_specs=(P("leaf", "rhs"), P("leaf", "rhs", None))
        + (P("leaf", None, None),) * 11,
        out_specs=P("leaf", "rhs"),
        check_vma=False,
    )
```
